32 devices in a mesh: dp: 8 (over z, x), expert: 4 (over y, core).
Axes of the slice: x: 2, y: 2, z: 4, core: 2. Of those that a mesh axis runs over, the one named last changes fastest.
Arguments:
- local_grads: bfloat16 [8, 4, 4, 524288], P('dp', 'expert')
- master_weights: float32 [4, 4, 524288], P('expert', None, 'dp'), may hold values from -6 to 6
- first_moment: float32 [4, 4, 524288], P('expert', None, 'dp')
- second_moment: float32 [4, 4, 524288], P('expert', None, 'dp')
Outputs:
- new_params: bfloat16 [4, 4, 524288], P('expert')
- new_master: float32 [4, 4, 524288], P('expert', None, 'dp')
- new_first: float32 [4, 4, 524288], P('expert', None, 'dp')
- new_second: float32 [4, 4, 524288], P('expert', None, 'dp')
The draws below stay inside these ranges and needn't reach their ends.
All inputs are finite; a program needn't handle non-finite values.
Results may differ from the reference program's by a relative error of at most 0.0013.
Values may be sent and summed in bfloat16 or wider, within the bound.
A program may use at most 128 MiB of HBM per device.

```python
import jax
import jax.numpy as jnp
from jax import lax

LAYERS = 4
SHARD = 65536
EXPERTS = 4
FLAT = 524288
N_DP = 8


def unit_scale():
    return (EXPERTS * LAYERS * FLAT) ** (-0.5)


def profile_gains(key, block_top, jitter):
    replicas = FLAT // SHARD
    block_count = replicas * 4
    expert_rise = 1.0 + 2.0 * jnp.arange(EXPERTS, dtype=jnp.float32) / max(EXPERTS - 1, 1)
    expert_jitter = jnp.exp(jax.random.uniform(jax.random.fold_in(key, 11), (EXPERTS,), jnp.float32, -jitter, jitter))
    block_rise = 1.0 + block_top * jnp.arange(block_count, dtype=jnp.float32) / max(block_count - 1, 1)
    block_jitter = jnp.exp(jax.random.uniform(jax.random.fold_in(key, 12), (EXPERTS, LAYERS, block_count), jnp.float32, -jitter, jitter))
    blocks = (expert_rise * expert_jitter).reshape(EXPERTS, 1, 1) * block_rise.reshape(1, 1, block_count) * block_jitter
    return jnp.repeat(blocks, SHARD // 4, axis=2)


def draw_local_grads(key, part):
    replicas = FLAT // SHARD
    shape = (replicas, EXPERTS, LAYERS, FLAT)
    rough = jax.random.uniform(jax.random.fold_in(key, 7), (EXPERTS, LAYERS, FLAT), jnp.float32, 0.5, 1.5)
    gains = profile_gains(key, 2.0, 0.7)
    common = jax.random.normal(jax.random.fold_in(key, 3), (EXPERTS, LAYERS, FLAT), jnp.float32)
    single = jax.random.normal(jax.random.fold_in(key, 4), shape, jnp.float32)
    spread = 60.0
    centered = single - jnp.mean(single, axis=0, keepdims=True)
    values = (common[None] + spread * centered) * (gains * rough * unit_scale())[None]
    return values.astype(jnp.bfloat16)


def draw_first_moment(key, part):
    shape = (EXPERTS, LAYERS, FLAT)
    values = 0.3 * jax.random.normal(key, shape, jnp.float32)
    return values * unit_scale()


def draw_second_moment(key, part):
    shape = (EXPERTS, LAYERS, FLAT)
    low = 0.1
    logs = jax.random.uniform(key, shape, jnp.float32, jnp.log(low), 0.0)
    return jnp.exp(logs) * unit_scale() ** 2


def levels(own_key, extent, split, low, high):
    factor_of, own = 1.0, jax.random.fold_in(own_key, 6)
    for axis_at, shards_of in split:
        steps = jnp.exp(jax.random.uniform(jax.random.fold_in(own, axis_at), (shards_of,), jnp.float32, low / len(split), high / len(split)))
        factor_of = factor_of * jnp.repeat(steps, extent[axis_at] // shards_of).reshape([-1 if axis == axis_at else 1 for axis in range(len(extent))])
    return factor_of


def gaussian(own_key, shape, scale, bound, pieces=(), kind=jnp.bfloat16):
    gain = levels(own_key, shape, pieces, -0.22, 0.18) if pieces else 1.0
    result = jax.random.normal(own_key, shape, jnp.float32) * scale * gain
    return jnp.minimum(jnp.maximum(result, -bound), bound).astype(kind)


def setup_inputs(seed: int = 0) -> dict:
    key_of = jax.random.split(jax.random.key(seed), 5)
    local_grads = draw_local_grads(jax.random.fold_in(key_of[4], 71), 0)
    master_weights = gaussian(key_of[1], (EXPERTS, LAYERS, FLAT), 1.0, 6.0, ((0, 4), (2, 8)), jnp.float32)
    first_moment = draw_first_moment(jax.random.fold_in(key_of[4], 71), 0)
    second_moment = draw_second_moment(jax.random.fold_in(key_of[4], 71), 0)
    return dict(local_grads=local_grads, master_weights=master_weights, first_moment=first_moment, second_moment=second_moment)


beta_first = 0.9
beta_second = 0.95
correct_first = 1.0 - 0.9 ** 10
correct_second = 1.0 - 0.95 ** 10
learn_rate = 0.05
decay_rate = 0.1
clip_limit = 1.0
tiny_eps = 1e-08
norm_eps = 1e-06

def adam_update(gradient, master, first, second, clip_factor):
    scaled = clip_factor * gradient
    new_first = beta_first * first + (1.0 - beta_first) * scaled
    new_second = beta_second * second + (1.0 - beta_second) * scaled * scaled
    direction = new_first / correct_first / (jnp.sqrt(new_second / correct_second) + tiny_eps)
    new_master = master - learn_rate * (decay_rate * master + direction)
    return (new_master, new_first, new_second)

def reference(local_grads, master_weights, first_moment, second_moment):
    mean_grad = lax.optimization_barrier(jnp.sum(local_grads.astype(jnp.float32), axis=0)) / N_DP
    grad_norm = jnp.sqrt(jnp.sum(mean_grad * mean_grad))
    clip_factor = jnp.minimum(1.0, clip_limit / (grad_norm + norm_eps))
    new_master, new_first, new_second = adam_update(mean_grad, master_weights, first_moment, second_moment, clip_factor)
    return (new_master.astype(jnp.bfloat16), new_master, new_first, new_second)
```

```python
import functools

import jax
import jax.numpy as jnp
from jax import lax
from jax.experimental import pallas as pl
from jax.experimental.pallas import tpu as pltpu
from jax.sharding import PartitionSpec as P

beta_first = 0.9
beta_second = 0.95
correct_first = 1.0 - 0.9**10
correct_second = 1.0 - 0.95**10
learn_rate = 0.05
decay_rate = 0.1
clip_limit = 1.0
tiny_eps = 1e-08
norm_eps = 1e-06

MESH = pl.DeviceIdType.MESH
F32 = jnp.float32
CHUNKS = 8
HALF = CHUNKS // 2
PIECES = 8
SPARE_BYTES = 4 * 1024 * 1024
BLOCK = 2048
SPAN = 250.0
TINY = 1e-35


def adam_update(gradient, master, first, second, clip_factor):
    scaled = clip_factor * gradient
    new_first = beta_first * first + (1.0 - beta_first) * scaled
    new_second = beta_second * second + (1.0 - beta_second) * scaled * scaled
    direction = new_first / correct_first / (jnp.sqrt(new_second / correct_second) + tiny_eps)
    new_master = master - learn_rate * (decay_rate * master + direction)
    return (new_master, new_first, new_second)


def spread_lanes(tile):
    return jnp.concatenate([tile] * (BLOCK // 128), axis=1)


def lane_peak(values):
    peak = jnp.abs(values)
    while peak.shape[1] > 128:
        half = peak.shape[1] // 2
        peak = jnp.maximum(peak[:, :half], peak[:, half:])
    return peak


def encode(values, scale):
    size = jnp.exp2(jnp.abs(values) * scale - SPAN / 2)
    return jnp.where(values < 0, -size, size).astype(jnp.bfloat16)


def decode(codes, peak):
    codes = codes.astype(F32)
    size = (jnp.log2(jnp.abs(codes)) + SPAN / 2) * spread_lanes(peak.astype(F32) / SPAN)
    return jnp.where(codes < 0, -size, size)


def kernel(
    Z, X, E, share,
    grads, master_in, first_in, second_in,
    gathered, master, first, second,
    own, xr, low, high, code, exact, mean_grad, norms, norms2,
    own_sem, state_sem, x_send, x_recv, z_send, low_recv, high_recv,
    n_send, n_recv, m_send, m_recv, g_send, g_recv, h_send,
):
    n = Z * X
    dp = lax.axis_index("dp")
    ex = lax.axis_index("expert")
    z, x = dp // X, dp % X
    chunk = share // CHUNKS

    def at_dp(zz, xx):
        return (zz * X + xx, ex)

    def lanes(base, size):
        return pl.ds(pl.multiple_of(base, 128), size)

    barrier = pltpu.get_barrier_semaphore()
    for k in range(1, n):
        pl.semaphore_signal(barrier, inc=1, device_id=((dp + k) % n, ex), device_id_type=MESH)
    for k in range(1, E):
        pl.semaphore_signal(barrier, inc=1, device_id=(dp, (ex + k) % E), device_id_type=MESH)
    pl.semaphore_wait(barrier, n - 1 + E - 1)

    def own_copy(zz):
        return pltpu.make_async_copy(
            grads.at[:, lanes((zz * X + x) * share, share)], own.at[zz], own_sem.at[zz]
        )

    def x_copy(zz, k, c):
        to = (x + k) % X
        return pltpu.make_async_remote_copy(
            src_ref=grads.at[:, lanes((zz * X + to) * share + c * chunk, chunk)],
            dst_ref=xr.at[zz, k - 1, :, lanes(c * chunk, chunk)],
            send_sem=x_send.at[zz, k - 1, c],
            recv_sem=x_recv.at[zz, k - 1, c],
            device_id=at_dp(z, to),
            device_id_type=MESH,
        )

    def for_dest(k, act):
        @pl.when(z + k < Z)
        def _():
            act(z + k)

        if k:
            @pl.when(z - k >= 0)
            def _():
                act(z - k)

    def start_first(zz):
        own_copy(zz).start()

        def body(c, carry):
            for k in range(1, X):
                x_copy(zz, k, c).start()
            return carry

        lax.fori_loop(0, CHUNKS, body, 0)

    for k in range(Z - 1, -1, -1):
        for_dest(k, start_first)
    states = [
        pltpu.make_async_copy(a, b, state_sem.at[i])
        for i, (a, b) in enumerate(((master_in, master), (first_in, first), (second_in, second)))
    ]
    for s in states:
        s.start()

    def z_copy(zz, c, up):
        return pltpu.make_async_remote_copy(
            src_ref=code.at[zz, c],
            dst_ref=(low if up else high).at[zz, c],
            send_sem=z_send.at[zz, c],
            recv_sem=(low_recv if up else high_recv).at[zz, c],
            device_id=at_dp(z + 1 if up else z - 1, x),
            device_id_type=MESH,
        )

    def sum_block(zz, c, b, extras):
        where = lanes(c * chunk + b * BLOCK, BLOCK)
        total = own[zz, :, where].astype(F32)
        for k in range(1, X):
            total = total + xr[zz, k - 1, :, where].astype(F32)
        for r in extras:
            total = total + decode(r[zz, c, :, lanes(b * BLOCK, BLOCK)], r[zz, c, :, pl.ds(chunk, 128)])
        return total

    def add_chunk(zz, c, extras):
        def add(b, peak):
            total = sum_block(zz, c, b, extras)
            exact[:, lanes(b * BLOCK, BLOCK)] = total
            return jnp.maximum(peak, lane_peak(total))

        peak = lax.fori_loop(0, chunk // BLOCK, add, jnp.zeros((own.shape[1], 128), F32))
        peak = (jnp.maximum(peak, TINY) * 1.01).astype(jnp.bfloat16)
        code[zz, c, :, pl.ds(chunk, 128)] = peak
        scale = spread_lanes(SPAN / peak.astype(F32))

        def write(b, carry):
            where = lanes(b * BLOCK, BLOCK)
            code[zz, c, :, where] = encode(exact[:, where], scale)
            return carry

        lax.fori_loop(0, chunk // BLOCK, write, 0)

    def hop(zz, c, up):
        for k in range(1, X):
            x_copy(zz, k, c).wait_recv()
        edge = z == (0 if up else Z - 1)

        @pl.when(edge)
        def _():
            add_chunk(zz, c, ())

        @pl.when(jnp.logical_not(edge))
        def _():
            z_copy(zz, c, up).wait_recv()
            add_chunk(zz, c, (low if up else high,))

        z_copy(zz, c, up).start()

    for k in range(Z - 1, 0, -1):
        for_dest(k, lambda zz: own_copy(zz).wait())

        def body(c, carry, k=k):
            @pl.when(z + k < Z)
            def _():
                hop(z + k, c, True)

            @pl.when(z - k >= 0)
            def _():
                hop(z - k, c, False)

            return carry

        lax.fori_loop(0, CHUNKS, body, 0)

    own_copy(z).wait()
    norms2[0] = jnp.zeros((8, 128), F32)

    def finish_chunk(c, extras):
        def body(b, carry):
            mean = sum_block(z, c, b, extras) / n
            mean_grad[:, lanes(c * chunk + b * BLOCK, BLOCK)] = mean
            return carry + mean * mean

        squares = lax.fori_loop(0, chunk // BLOCK, body, jnp.zeros((own.shape[1], BLOCK), F32))
        norms2[0] = norms2[0] + jnp.full((8, 128), jnp.sum(squares), F32)

    def finish(c, carry):
        for k in range(1, X):
            x_copy(z, k, c).wait_recv()

        @pl.when(z > 0)
        def _():
            z_copy(z, c, True).wait_recv()

        @pl.when(z < Z - 1)
        def _():
            z_copy(z, c, False).wait_recv()

        @pl.when(z == 0)
        def _():
            finish_chunk(c, (high,))

        @pl.when(z == Z - 1)
        def _():
            finish_chunk(c, (low,))

        @pl.when(jnp.logical_and(z > 0, z < Z - 1))
        def _():
            finish_chunk(c, (low, high))

        return carry

    lax.fori_loop(0, CHUNKS, finish, 0)

    norms[0] = norms2[0]

    def n_copy(k):
        return pltpu.make_async_remote_copy(
            src_ref=norms.at[0], dst_ref=norms.at[k],
            send_sem=n_send.at[k], recv_sem=n_recv.at[k],
            device_id=((dp + k) % n, ex), device_id_type=MESH,
        )

    def m_copy(k):
        return pltpu.make_async_remote_copy(
            src_ref=norms2.at[0], dst_ref=norms2.at[k],
            send_sem=m_send.at[k], recv_sem=m_recv.at[k],
            device_id=(dp, (ex + k) % E), device_id_type=MESH,
        )

    for k in range(1, n):
        n_copy(k).start()
    for s in states:
        s.wait()
    total = norms[0]
    for k in range(1, n):
        n_copy(k).wait_recv()
        total = total + norms[k]
    norms2[0] = total
    for k in range(1, E):
        m_copy(k).start()
    for k in range(1, E):
        m_copy(k).wait_recv()
        total = total + norms2[k]
    clip_all = jnp.minimum(1.0, clip_limit / (jnp.sqrt(total) + norm_eps))
    clip_factor = jnp.max(clip_all)

    def g_copy(zz, c, way):
        where = lanes((zz * X + x) * share + c * chunk, chunk)
        if way < 2:
            target = at_dp(z + 1 if way == 0 else z - 1, x)
        else:
            target = at_dp(z, (x + way - 1) % X)
        return pltpu.make_async_remote_copy(
            src_ref=gathered.at[:, where], dst_ref=gathered.at[:, where],
            send_sem=g_send.at[way, zz, c], recv_sem=g_recv.at[zz * X + x, c],
            device_id=target, device_id_type=MESH,
        )

    def arrived(zz, xx, c):
        where = lanes((zz * X + xx) * share + c * chunk, chunk)
        pltpu.make_async_remote_copy(
            src_ref=gathered.at[:, where], dst_ref=gathered.at[:, where],
            send_sem=g_send.at[0, 0, c], recv_sem=g_recv.at[zz * X + xx, c],
            device_id=(dp, (ex + 1) % E), device_id_type=MESH,
        ).wait_recv()

    pair = z + 1 - 2 * (z % 2)

    def h_copy(k, c):
        where = lanes((z * X + (x + k) % X) * share + c * chunk, chunk)
        return pltpu.make_async_remote_copy(
            src_ref=gathered.at[:, where], dst_ref=gathered.at[:, where],
            send_sem=h_send.at[k - 1, c], recv_sem=g_recv.at[z * X + (x + k) % X, c],
            device_id=at_dp(pair, x), device_id_type=MESH,
        )

    def along_x(zz, c, act):
        @pl.when(jnp.logical_or(zz != pair, c < HALF))
        def _():
            for k in range(1, X):
                act(g_copy(zz, c, k + 1))

    def update(c, carry):
        def body(b, inner):
            where = lanes(c * chunk + b * BLOCK, BLOCK)
            m, f, s = adam_update(
                mean_grad[:, where], master[:, where], first[:, where], second[:, where], clip_factor
            )
            master[:, where] = m
            first[:, where] = f
            second[:, where] = s
            gathered[:, lanes(dp * share + c * chunk + b * BLOCK, BLOCK)] = m.astype(jnp.bfloat16)
            return inner

        lax.fori_loop(0, chunk // BLOCK, body, 0)

        @pl.when(z < Z - 1)
        def _():
            g_copy(z, c, 0).start()

        @pl.when(z > 0)
        def _():
            g_copy(z, c, 1).start()

        for k in range(1, X):
            g_copy(z, c, k + 1).start()
        return carry

    lax.fori_loop(0, CHUNKS, update, 0)

    for s in range(1, Z):
        def relay(c, carry, s=s):
            @pl.when(z - s >= 0)
            def _():
                arrived(z - s, x, c)

                @pl.when(z < Z - 1)
                def _():
                    g_copy(z - s, c, 0).start()

                along_x(z - s, c, lambda copy: copy.start())

            @pl.when(z + s < Z)
            def _():
                arrived(z + s, x, c)

                @pl.when(z > 0)
                def _():
                    g_copy(z + s, c, 1).start()

                along_x(z + s, c, lambda copy: copy.start())

            return carry

        lax.fori_loop(0, CHUNKS, relay, 0)

        if s == 1:
            def across(c, carry):
                for k in range(1, X):
                    arrived(z, (x + k) % X, c)
                    h_copy(k, c).start()
                return carry

            lax.fori_loop(HALF, CHUNKS, across, 0)

    for s in range(Z):
        def collect(zz, s=s):
            def body(c, carry):
                for k in range(1, X):
                    arrived(zz, (x + k) % X, c)
                return carry

            lax.fori_loop(0, HALF if s == 0 else CHUNKS, body, 0)

        for_dest(s, collect)

    def drain(c, carry):
        for zz in range(Z):
            for k in range(1, X):
                x_copy(zz, k, c).wait_send()
            along_x(zz, c, lambda copy: copy.wait_send())

            @pl.when(zz > z)
            def _():
                z_copy(zz, c, True).wait_send()

            @pl.when(zz < z)
            def _():
                z_copy(zz, c, False).wait_send()

            @pl.when(jnp.logical_and(zz <= z, z < Z - 1))
            def _():
                g_copy(zz, c, 0).wait_send()

            @pl.when(jnp.logical_and(zz >= z, z > 0))
            def _():
                g_copy(zz, c, 1).wait_send()

        @pl.when(c >= HALF)
        def _():
            for k in range(1, X):
                h_copy(k, c).wait_send()

        return carry

    lax.fori_loop(0, CHUNKS, drain, 0)
    for k in range(1, n):
        n_copy(k).wait_send()
    for k in range(1, E):
        m_copy(k).wait_send()


def write_out(count, *refs):
    sources, targets, sem = refs[:count], refs[count : 2 * count], refs[2 * count]

    def copies(i):
        size = sources[i].shape[1] // PIECES
        for p in range(PIECES):
            where = pl.ds(p * size, size)
            yield pltpu.make_async_copy(sources[i].at[:, where], targets[i].at[:, where], sem.at[i, p])

    for i in range(count):
        for copy in copies(i):
            copy.start()
    for i in range(count):
        for copy in copies(i):
            copy.wait()


def split(count):
    rows = 1
    while rows * rows < count:
        rows *= 2
    return rows, count // rows


def shards(Z, X, E, local_grads, master_weights, first_moment, second_moment):
    layers, flat = local_grads.shape[2:]
    n = Z * X
    share = flat // n
    whole = pl.BlockSpec(memory_space=pltpu.HBM)
    piece = jax.ShapeDtypeStruct((layers, share), F32)
    dma = pltpu.SemaphoreType.DMA
    local = pl.BlockSpec(memory_space=pltpu.VMEM)
    shapes = (jax.ShapeDtypeStruct((layers, flat), jnp.bfloat16), piece, piece, piece)
    arrays = (local_grads[0, 0], master_weights[0], first_moment[0], second_moment[0])
    out_bytes = layers * (2 * flat + 3 * 4 * share)
    used_bytes = layers * Z * share * (2 * X + 3 * 2) + layers * share * 4 + out_bytes
    results = pl.pallas_call(
        functools.partial(kernel, Z, X, E, share),
        out_shape=shapes,
        in_specs=[whole] * 4,
        out_specs=(local,) * 4,
        scratch_shapes=[
            pltpu.VMEM((Z, layers, share), jnp.bfloat16),
            pltpu.VMEM((Z, X - 1, layers, share), jnp.bfloat16),
            pltpu.VMEM((Z, CHUNKS, layers, share // CHUNKS + 128), jnp.bfloat16),
            pltpu.VMEM((Z, CHUNKS, layers, share // CHUNKS + 128), jnp.bfloat16),
            pltpu.VMEM((Z, CHUNKS, layers, share // CHUNKS + 128), jnp.bfloat16),
            pltpu.VMEM((layers, share // CHUNKS), F32),
            pltpu.VMEM((layers, share), F32),
            pltpu.VMEM((n, 8, 128), F32),
            pltpu.VMEM((E, 8, 128), F32),
            dma((Z,)), dma((3,)),
            dma((Z, X - 1, CHUNKS)), dma((Z, X - 1, CHUNKS)),
            dma((Z, CHUNKS)), dma((Z, CHUNKS)), dma((Z, CHUNKS)),
            dma((n,)), dma((n,)), dma((E,)), dma((E,)),
            dma((X + 1, Z, CHUNKS)), dma((n, CHUNKS)), dma((X - 1, CHUNKS)),
        ],
        compiler_params=pltpu.CompilerParams(
            collective_id=0, has_side_effects=True, vmem_limit_bytes=used_bytes + SPARE_BYTES
        ),
    )(*(pltpu.with_memory_space_constraint(a, pltpu.HBM) for a in arrays))
    results = pl.pallas_call(
        functools.partial(write_out, len(shapes)),
        out_shape=shapes,
        in_specs=[local] * 4,
        out_specs=(whole,) * 4,
        scratch_shapes=[dma((len(shapes), PIECES))],
        compiler_params=pltpu.CompilerParams(vmem_limit_bytes=out_bytes + SPARE_BYTES),
    )(*results)
    return tuple(r[None] for r in results)


def solution(mesh):
    Z, X = split(mesh.shape["dp"])
    moments = P("expert", None, "dp")
    return jax.shard_map(
        functools.partial(shards, Z, X, mesh.shape["expert"]),
        mesh=mesh,
        in_specs=(P("dp", "expert", None, None), moments, moments, moments),
        out_specs=(P("expert", None, None), moments, moments, moments),
        check_vma=False,
    )
```

```python
import functools

import jax
import jax.numpy as jnp
from jax import lax
from jax.experimental import pallas as pl
from jax.experimental.pallas import tpu as pltpu
from jax.sharding import PartitionSpec as P

beta_first = 0.9
beta_second = 0.95
correct_first = 1.0 - 0.9**10
correct_second = 1.0 - 0.95**10
learn_rate = 0.05
decay_rate = 0.1
clip_limit = 1.0
tiny_eps = 1e-08
norm_eps = 1e-06

MESH = pl.DeviceIdType.MESH
F32 = jnp.float32
CHUNKS = 8
HALF = CHUNKS // 2
PIECES = 8
SPARE_BYTES = 4 * 1024 * 1024
BLOCK = 2048
SPAN = 250.0
TINY = 1e-35


def adam_update(gradient, master, first, second, clip_factor):
    scaled = clip_factor * gradient
    new_first = beta_first * first + (1.0 - beta_first) * scaled
    new_second = beta_second * second + (1.0 - beta_second) * scaled * scaled
    direction = new_first / correct_first / (jnp.sqrt(new_second / correct_second) + tiny_eps)
    new_master = master - learn_rate * (decay_rate * master + direction)
    return (new_master, new_first, new_second)


def spread_lanes(tile):
    return jnp.concatenate([tile] * (BLOCK // 128), axis=1)


def lane_peak(values):
    peak = jnp.abs(values)
    while peak.shape[1] > 128:
        half = peak.shape[1] // 2
        peak = jnp.maximum(peak[:, :half], peak[:, half:])
    return peak


def encode(values, scale):
    size = jnp.exp2(jnp.abs(values) * scale - SPAN / 2)
    return jnp.where(values < 0, -size, size).astype(jnp.bfloat16)


def decode(codes, peak):
    codes = codes.astype(F32)
    size = (jnp.log2(jnp.abs(codes)) + SPAN / 2) * spread_lanes(peak.astype(F32) / SPAN)
    return jnp.where(codes < 0, -size, size)


def kernel(
    Z, X, E, share,
    grads, master_in, first_in, second_in,
    gathered, master, first, second,
    own, side, xr, pr, xc, raw, chain, code, xcode, exact, mean_grad, norms, norms2,
    own_sem, state_sem, x_send, x_recv, z_send, z_recv,
    p_send, p_recv, q_send, q_recv, r_send, r_recv,
    n_send, n_recv, m_send, m_recv, g_send, g_recv, h_send,
):
    n = Z * X
    dp = lax.axis_index("dp")
    ex = lax.axis_index("expert")
    z, x = dp // X, dp % X
    chunk = share // CHUNKS

    def at_dp(zz, xx):
        return (zz * X + xx, ex)

    def lanes(base, size):
        return pl.ds(pl.multiple_of(base, 128), size)

    pair = z + 1 - 2 * (z % 2)
    edge = jnp.logical_or(z == 0, z == Z - 1)
    inside = jnp.logical_not(edge)

    def own_copy(zz):
        return pltpu.make_async_copy(
            grads.at[:, lanes((zz * X + x) * share, share)], own.at[zz], own_sem.at[zz]
        )

    def side_copy(k):
        start = (z * X + (x + k) % X) * share + HALF * chunk
        return pltpu.make_async_copy(
            grads.at[:, lanes(start, HALF * chunk)], side.at[k - 1], own_sem.at[Z + k - 1]
        )

    states = [
        pltpu.make_async_copy(a, b, state_sem.at[i])
        for i, (a, b) in enumerate(((master_in, master), (first_in, first), (second_in, second)))
    ]

    barrier = pltpu.get_barrier_semaphore()

    def greet(device):
        pl.semaphore_signal(barrier, inc=1, device_id=device, device_id_type=MESH)

    for k in range(1, X):
        greet(at_dp(z, (x + k) % X))
    for k in range(1, E):
        greet((dp, (ex + k) % E))

    @pl.when(z > 0)
    def _():
        greet(at_dp(z - 1, x))

    @pl.when(z < Z - 1)
    def _():
        greet(at_dp(z + 1, x))

    pl.semaphore_wait(barrier, X + E - jnp.where(edge, 1, 0))

    def x_copy(zz, k, c):
        to = (x + k) % X
        return pltpu.make_async_remote_copy(
            src_ref=grads.at[:, lanes((zz * X + to) * share + c * chunk, chunk)],
            dst_ref=xr.at[zz, k - 1, :, lanes(c * chunk, chunk)],
            send_sem=x_send.at[zz, k - 1, c],
            recv_sem=x_recv.at[zz, k - 1, c],
            device_id=at_dp(z, to),
            device_id_type=MESH,
        )

    def p_copy(k, c):
        return pltpu.make_async_remote_copy(
            src_ref=grads.at[:, lanes((pair * X + (x + k) % X) * share + c * chunk, chunk)],
            dst_ref=pr.at[k - 1, :, lanes((c - HALF) * chunk, chunk)],
            send_sem=p_send.at[k - 1, c - HALF],
            recv_sem=p_recv.at[k - 1, c - HALF],
            device_id=at_dp(pair, x),
            device_id_type=MESH,
        )

    def q_copy(k, c):
        return pltpu.make_async_remote_copy(
            src_ref=xcode.at[k - 1, c - HALF],
            dst_ref=xc.at[k - 1, c - HALF],
            send_sem=q_send.at[k - 1, c - HALF],
            recv_sem=q_recv.at[k - 1, c - HALF],
            device_id=at_dp(z, (x + k) % X),
            device_id_type=MESH,
        )

    def r_copy(c):
        return pltpu.make_async_remote_copy(
            src_ref=grads.at[:, lanes((pair * X + x) * share + c * chunk, chunk)],
            dst_ref=raw.at[:, lanes((c - HALF) * chunk, chunk)],
            send_sem=r_send.at[c - HALF],
            recv_sem=r_recv.at[c - HALF],
            device_id=at_dp(pair, x),
            device_id_type=MESH,
        )

    def z_copy(zz, c):
        up = jnp.where(zz > z, 1, 0)
        return pltpu.make_async_remote_copy(
            src_ref=code.at[zz, c],
            dst_ref=chain.at[up, zz, c],
            send_sem=z_send.at[zz, c],
            recv_sem=z_recv.at[up, zz, c],
            device_id=at_dp(z - 1 + 2 * up, x),
            device_id_type=MESH,
        )

    def from_chain(up, zz, c):
        return pltpu.make_async_remote_copy(
            src_ref=code.at[zz, c],
            dst_ref=chain.at[up, zz, c],
            send_sem=z_send.at[zz, c],
            recv_sem=z_recv.at[up, zz, c],
            device_id=at_dp(z, (x + 1) % X),
            device_id_type=MESH,
        )

    def for_dest(k, act):
        @pl.when(z + k < Z)
        def _():
            act(z + k)

        if k:
            @pl.when(z - k >= 0)
            def _():
                act(z - k)

    def start_first(zz):
        own_copy(zz).start()
        near = jnp.logical_or(zz == z, zz == pair)

        def body(c, carry):
            for k in range(1, X):
                x_copy(zz, k, c).start()
            return carry

        lax.fori_loop(0, jnp.where(near, HALF, CHUNKS), body, 0)

    def over_late(act):
        def body(c, carry):
            act(c)
            return carry

        lax.fori_loop(HALF, CHUNKS, body, 0)

    @over_late
    def _(c):
        for k in range(1, X):
            p_copy(k, c).start()

    for k in range(Z - 1, -1, -1):
        for_dest(k, start_first)
    for k in range(1, X):
        side_copy(k).start()
    for s in states:
        s.start()

    def part(ref, c, b):
        return ref[:, lanes(c * chunk + b * BLOCK, BLOCK)].astype(F32)

    def unpack(ref, b):
        return decode(ref[:, lanes(b * BLOCK, BLOCK)], ref[:, pl.ds(chunk, 128)])

    def pack(ref, block_sum):
        def add(b, peak):
            total = block_sum(b)
            exact[:, lanes(b * BLOCK, BLOCK)] = total
            return jnp.maximum(peak, lane_peak(total))

        peak = lax.fori_loop(0, chunk // BLOCK, add, jnp.zeros((own.shape[1], 128), F32))
        peak = (jnp.maximum(peak, TINY) * 1.01).astype(jnp.bfloat16)
        ref[:, pl.ds(chunk, 128)] = peak
        scale = spread_lanes(SPAN / peak.astype(F32))

        def write(b, carry):
            where = lanes(b * BLOCK, BLOCK)
            ref[:, where] = encode(exact[:, where], scale)
            return carry

        lax.fori_loop(0, chunk // BLOCK, write, 0)

    def gather_sum(zz, c, with_x, ups):
        def block_sum(b):
            total = part(own.at[zz], c, b)
            if with_x:
                for k in range(1, X):
                    total = total + part(xr.at[zz, k - 1], c, b)
            for up in ups:
                total = total + unpack(chain.at[up, zz, c], b)
            return total

        return block_sum

    def hop(zz, c):
        late = jnp.logical_and(zz == pair, c >= HALF)
        up = jnp.where(zz > z, 1, 0)
        first = z == (1 - up) * (Z - 1)
        later = jnp.logical_not(first)

        @pl.when(jnp.logical_not(late))
        def _():
            for k in range(1, X):
                x_copy(zz, k, c).wait_recv()

        @pl.when(later)
        def _():
            from_chain(up, zz, c).wait_recv()

        @pl.when(jnp.logical_and(first, jnp.logical_not(late)))
        def _():
            pack(code.at[zz, c], gather_sum(zz, c, True, ()))

        @pl.when(jnp.logical_and(later, jnp.logical_not(late)))
        def _():
            pack(code.at[zz, c], gather_sum(zz, c, True, (up,)))

        @pl.when(jnp.logical_and(later, late))
        def _():
            pack(code.at[zz, c], gather_sum(zz, c, False, (up,)))

        @pl.when(jnp.logical_not(jnp.logical_and(first, late)))
        def _():
            z_copy(zz, c).start()

    for k in range(Z - 1, 0, -1):
        for_dest(k, lambda zz: own_copy(zz).wait())
        lower, upper = z - k >= 0, z + k < Z
        count = jnp.where(lower, 1, 0) + jnp.where(upper, 1, 0)

        def body(i, carry, k=k, upper=upper, count=count):
            goes_up = jnp.logical_and(upper, i % count == 0)
            hop(jnp.where(goes_up, z + k, z - k), i // count)
            return carry

        @pl.when(count > 0)
        def _(body=body, count=count):
            lax.fori_loop(0, CHUNKS * count, body, 0)

        if k == Z - 1:
            @pl.when(edge)
            def _():
                over_late(lambda c: r_copy(c).start())

            for j in range(1, X):
                side_copy(j).wait()

            @over_late
            def _(c):
                for j in range(1, X):
                    p_copy(j, c).wait_recv()
                    pack(
                        xcode.at[j - 1, c - HALF],
                        lambda b: part(side.at[j - 1], c - HALF, b) + part(pr.at[j - 1], c - HALF, b),
                    )
                    q_copy(j, c).start()

    own_copy(z).wait()
    norms2[0] = jnp.zeros((8, 128), F32)

    def finish_chunk(c, block_sum):
        def body(b, carry):
            mean = block_sum(b) / n
            mean_grad[:, lanes(c * chunk + b * BLOCK, BLOCK)] = mean
            return carry + mean * mean

        squares = lax.fori_loop(0, chunk // BLOCK, body, jnp.zeros((own.shape[1], BLOCK), F32))
        norms2[0] = norms2[0] + jnp.full((8, 128), jnp.sum(squares), F32)

    def late_sum(c, ups, with_raw):
        chained = gather_sum(z, c, False, ups)

        def block_sum(b):
            total = chained(b)
            for k in range(1, X):
                total = total + unpack(xc.at[k - 1, c - HALF], b)
            if with_raw:
                total = total + part(raw, c - HALF, b)
            return total

        return block_sum

    far = jnp.where(pair < z, 0, 1)
    far = jnp.where(edge, jnp.where(z == 0, 0, 1), far)
    raw_pair = jnp.logical_and(inside, jnp.logical_or(pair == 0, pair == Z - 1))
    both_pair = jnp.logical_and(inside, jnp.logical_not(raw_pair))

    def early_finish(c):
        for k in range(1, X):
            x_copy(z, k, c).wait_recv()

        @pl.when(edge)
        def _():
            from_chain(far, z, c).wait_recv()
            finish_chunk(c, gather_sum(z, c, True, (far,)))

        @pl.when(inside)
        def _():
            for up in range(2):
                from_chain(up, z, c).wait_recv()
            finish_chunk(c, gather_sum(z, c, True, (0, 1)))

    def late_finish(c):
        for k in range(1, X):
            q_copy(k, c).wait_recv()

        @pl.when(edge)
        def _():
            from_chain(far, z, c).wait_recv()
            finish_chunk(c, late_sum(c, (far,), False))

        @pl.when(raw_pair)
        def _():
            from_chain(far, z, c).wait_recv()
            r_copy(c).wait_recv()
            finish_chunk(c, late_sum(c, (far,), True))

        if Z > 4:
            @pl.when(both_pair)
            def _():
                for up in range(2):
                    from_chain(up, z, c).wait_recv()
                finish_chunk(c, late_sum(c, (0, 1), False))

    def finish(c, carry):
        early_finish(c)
        late_finish(c + HALF)
        return carry

    lax.fori_loop(0, HALF, finish, 0)

    norms[0] = norms2[0]

    def n_copy(k):
        return pltpu.make_async_remote_copy(
            src_ref=norms.at[0], dst_ref=norms.at[k],
            send_sem=n_send.at[k], recv_sem=n_recv.at[k],
            device_id=((dp + k) % n, ex), device_id_type=MESH,
        )

    def m_copy(k):
        return pltpu.make_async_remote_copy(
            src_ref=norms2.at[0], dst_ref=norms2.at[k],
            send_sem=m_send.at[k], recv_sem=m_recv.at[k],
            device_id=(dp, (ex + k) % E), device_id_type=MESH,
        )

    for k in range(1, n):
        n_copy(k).start()
    for s in states:
        s.wait()
    total = norms[0]
    for k in range(1, n):
        n_copy(k).wait_recv()
        total = total + norms[k]
    norms2[0] = total
    for k in range(1, E):
        m_copy(k).start()
    for k in range(1, E):
        m_copy(k).wait_recv()
        total = total + norms2[k]
    clip_all = jnp.minimum(1.0, clip_limit / (jnp.sqrt(total) + norm_eps))
    clip_factor = jnp.max(clip_all)

    def g_copy(zz, c, way):
        where = lanes((zz * X + x) * share + c * chunk, chunk)
        if way < 2:
            target = at_dp(z + 1 if way == 0 else z - 1, x)
        else:
            target = at_dp(z, (x + way - 1) % X)
        return pltpu.make_async_remote_copy(
            src_ref=gathered.at[:, where], dst_ref=gathered.at[:, where],
            send_sem=g_send.at[way, zz, c], recv_sem=g_recv.at[zz * X + x, c],
            device_id=target, device_id_type=MESH,
        )

    def arrived(zz, xx, c):
        where = lanes((zz * X + xx) * share + c * chunk, chunk)
        pltpu.make_async_remote_copy(
            src_ref=gathered.at[:, where], dst_ref=gathered.at[:, where],
            send_sem=g_send.at[0, 0, c], recv_sem=g_recv.at[zz * X + xx, c],
            device_id=(dp, (ex + 1) % E), device_id_type=MESH,
        ).wait_recv()

    def h_copy(k, c):
        where = lanes((z * X + (x + k) % X) * share + c * chunk, chunk)
        return pltpu.make_async_remote_copy(
            src_ref=gathered.at[:, where], dst_ref=gathered.at[:, where],
            send_sem=h_send.at[k - 1, c], recv_sem=g_recv.at[z * X + (x + k) % X, c],
            device_id=at_dp(pair, x), device_id_type=MESH,
        )

    def along_x(zz, c, act):
        @pl.when(jnp.logical_or(zz != pair, c < HALF))
        def _():
            for k in range(1, X):
                act(g_copy(zz, c, k + 1))

    def update(c, carry):
        def body(b, inner):
            where = lanes(c * chunk + b * BLOCK, BLOCK)
            m, f, s = adam_update(
                mean_grad[:, where], master[:, where], first[:, where], second[:, where], clip_factor
            )
            master[:, where] = m
            first[:, where] = f
            second[:, where] = s
            gathered[:, lanes(dp * share + c * chunk + b * BLOCK, BLOCK)] = m.astype(jnp.bfloat16)
            return inner

        lax.fori_loop(0, chunk // BLOCK, body, 0)

        @pl.when(z < Z - 1)
        def _():
            g_copy(z, c, 0).start()

        @pl.when(z > 0)
        def _():
            g_copy(z, c, 1).start()

        for k in range(1, X):
            g_copy(z, c, k + 1).start()
        return carry

    lax.fori_loop(0, CHUNKS, update, 0)

    for s in range(1, Z):
        def relay(c, carry, s=s):
            @pl.when(z - s >= 0)
            def _():
                arrived(z - s, x, c)

                @pl.when(z < Z - 1)
                def _():
                    g_copy(z - s, c, 0).start()

                along_x(z - s, c, lambda copy: copy.start())

            @pl.when(z + s < Z)
            def _():
                arrived(z + s, x, c)

                @pl.when(z > 0)
                def _():
                    g_copy(z + s, c, 1).start()

                along_x(z + s, c, lambda copy: copy.start())

            return carry

        lax.fori_loop(0, CHUNKS, relay, 0)

        if s == 1:
            def across(c, carry):
                for k in range(1, X):
                    arrived(z, (x + k) % X, c)
                    h_copy(k, c).start()
                return carry

            lax.fori_loop(HALF, CHUNKS, across, 0)

    for s in range(Z):
        def collect(zz, s=s):
            def body(c, carry):
                for k in range(1, X):
                    arrived(zz, (x + k) % X, c)
                return carry

            lax.fori_loop(0, HALF if s == 0 else CHUNKS, body, 0)

        for_dest(s, collect)

    def drain(c, carry):
        for zz in range(Z):
            near = jnp.logical_or(zz == z, zz == pair)

            @pl.when(jnp.logical_not(jnp.logical_and(near, c >= HALF)))
            def _():
                for k in range(1, X):
                    x_copy(zz, k, c).wait_send()

            along_x(zz, c, lambda copy: copy.wait_send())
            direct = jnp.logical_and(jnp.logical_and(edge, zz == pair), c >= HALF)

            @pl.when(jnp.logical_and(zz != z, jnp.logical_not(direct)))
            def _():
                z_copy(zz, c).wait_send()

            @pl.when(jnp.logical_and(zz <= z, z < Z - 1))
            def _():
                g_copy(zz, c, 0).wait_send()

            @pl.when(jnp.logical_and(zz >= z, z > 0))
            def _():
                g_copy(zz, c, 1).wait_send()

        @pl.when(c >= HALF)
        def _():
            for k in range(1, X):
                h_copy(k, c).wait_send()
                p_copy(k, c).wait_send()
                q_copy(k, c).wait_send()

        @pl.when(jnp.logical_and(c >= HALF, edge))
        def _():
            r_copy(c).wait_send()

        return carry

    lax.fori_loop(0, CHUNKS, drain, 0)
    for k in range(1, n):
        n_copy(k).wait_send()
    for k in range(1, E):
        m_copy(k).wait_send()


def write_out(count, *refs):
    sources, targets, sem = refs[:count], refs[count : 2 * count], refs[2 * count]

    def copies(i):
        size = sources[i].shape[1] // PIECES
        for p in range(PIECES):
            where = pl.ds(p * size, size)
            yield pltpu.make_async_copy(sources[i].at[:, where], targets[i].at[:, where], sem.at[i, p])

    for i in range(count):
        for copy in copies(i):
            copy.start()
    for i in range(count):
        for copy in copies(i):
            copy.wait()


def split(count):
    rows = 1
    while rows * rows < count:
        rows *= 2
    return rows, count // rows


def shards(Z, X, E, local_grads, master_weights, first_moment, second_moment):
    layers, flat = local_grads.shape[2:]
    n = Z * X
    share = flat // n
    whole = pl.BlockSpec(memory_space=pltpu.HBM)
    piece = jax.ShapeDtypeStruct((layers, share), F32)
    dma = pltpu.SemaphoreType.DMA
    local = pl.BlockSpec(memory_space=pltpu.VMEM)
    shapes = (jax.ShapeDtypeStruct((layers, flat), jnp.bfloat16), piece, piece, piece)
    arrays = (local_grads[0, 0], master_weights[0], first_moment[0], second_moment[0])
    out_bytes = layers * (2 * flat + 3 * 4 * share)
    coded = share // CHUNKS + 128
    used_bytes = layers * share * (Z * (2 * X + 3 * 2) + 4 * X + 5) + out_bytes
    results = pl.pallas_call(
        functools.partial(kernel, Z, X, E, share),
        out_shape=shapes,
        in_specs=[whole] * 4,
        out_specs=(local,) * 4,
        scratch_shapes=[
            pltpu.VMEM((Z, layers, share), jnp.bfloat16),
            pltpu.VMEM((X - 1, layers, share // 2), jnp.bfloat16),
            pltpu.VMEM((Z, X - 1, layers, share), jnp.bfloat16),
            pltpu.VMEM((X - 1, layers, share // 2), jnp.bfloat16),
            pltpu.VMEM((X - 1, HALF, layers, coded), jnp.bfloat16),
            pltpu.VMEM((layers, share // 2), jnp.bfloat16),
            pltpu.VMEM((2, Z, CHUNKS, layers, coded), jnp.bfloat16),
            pltpu.VMEM((Z, CHUNKS, layers, coded), jnp.bfloat16),
            pltpu.VMEM((X - 1, HALF, layers, coded), jnp.bfloat16),
            pltpu.VMEM((layers, share // CHUNKS), F32),
            pltpu.VMEM((layers, share), F32),
            pltpu.VMEM((n, 8, 128), F32),
            pltpu.VMEM((E, 8, 128), F32),
            dma((Z + X - 1,)), dma((3,)),
            dma((Z, X - 1, CHUNKS)), dma((Z, X - 1, CHUNKS)),
            dma((Z, CHUNKS)), dma((2, Z, CHUNKS)),
            dma((X - 1, HALF)), dma((X - 1, HALF)), dma((X - 1, HALF)), dma((X - 1, HALF)),
            dma((HALF,)), dma((HALF,)),
            dma((n,)), dma((n,)), dma((E,)), dma((E,)),
            dma((X + 1, Z, CHUNKS)), dma((n, CHUNKS)), dma((X - 1, CHUNKS)),
        ],
        compiler_params=pltpu.CompilerParams(
            collective_id=0, has_side_effects=True, vmem_limit_bytes=used_bytes + SPARE_BYTES
        ),
    )(*(pltpu.with_memory_space_constraint(a, pltpu.HBM) for a in arrays))
    results = pl.pallas_call(
        functools.partial(write_out, len(shapes)),
        out_shape=shapes,
        in_specs=[local] * 4,
        out_specs=(whole,) * 4,
        scratch_shapes=[dma((len(shapes), PIECES))],
        compiler_params=pltpu.CompilerParams(vmem_limit_bytes=out_bytes + SPARE_BYTES),
    )(*results)
    return tuple(r[None] for r in results)


def solution(mesh):
    Z, X = split(mesh.shape["dp"])
    moments = P("expert", None, "dp")
    return jax.shard_map(
        functools.partial(shards, Z, X, mesh.shape["expert"]),
        mesh=mesh,
        in_specs=(P("dp", "expert", None, None), moments, moments, moments),
        out_specs=(P("expert", None, None), moments, moments, moments),
        check_vma=False,
    )
```

```python
import functools

import jax
import jax.numpy as jnp
from jax import lax
from jax.experimental import pallas as pl
from jax.experimental.pallas import tpu as pltpu
from jax.sharding import PartitionSpec as P

beta_first = 0.9
beta_second = 0.95
correct_first = 1.0 - 0.9**10
correct_second = 1.0 - 0.95**10
learn_rate = 0.05
decay_rate = 0.1
clip_limit = 1.0
tiny_eps = 1e-08
norm_eps = 1e-06

MESH = pl.DeviceIdType.MESH
F32 = jnp.float32
CHUNKS = 4
HALF = CHUNKS // 2
SENDS = 4
SEND_HALF = SENDS // 2
PIECES = 8
SPARE_BYTES = 4 * 1024 * 1024
BLOCK = 2048
SPAN = 250.0
TINY = 1e-35


def adam_update(gradient, master, first, second, clip_factor):
    scaled = clip_factor * gradient
    new_first = beta_first * first + (1.0 - beta_first) * scaled
    new_second = beta_second * second + (1.0 - beta_second) * scaled * scaled
    direction = new_first / correct_first / (jnp.sqrt(new_second / correct_second) + tiny_eps)
    new_master = master - learn_rate * (decay_rate * master + direction)
    return (new_master, new_first, new_second)


def spread_lanes(tile):
    return jnp.concatenate([tile] * (BLOCK // 128), axis=1)


def lane_peak(values):
    peak = jnp.abs(values)
    while peak.shape[1] > 128:
        half = peak.shape[1] // 2
        peak = jnp.maximum(peak[:, :half], peak[:, half:])
    return peak


def encode(values, scale):
    size = jnp.exp2(jnp.abs(values) * scale - SPAN / 2)
    return jnp.where(values < 0, -size, size).astype(jnp.bfloat16)


def decode(codes, peak):
    codes = codes.astype(F32)
    size = (jnp.log2(jnp.abs(codes)) + SPAN / 2) * spread_lanes(peak.astype(F32) / SPAN)
    return jnp.where(codes < 0, -size, size)


def kernel(
    Z, X, E, share,
    grads, master_in, first_in, second_in,
    gathered, master, first, second,
    own, side, xr, pr, xc, raw, chain, code, xcode, exact, mean_grad, squares, norms,
    own_sem, state_sem, x_send, x_recv, z_send, z_recv,
    p_send, p_recv, q_send, q_recv, r_send, r_recv,
    n_send, n_recv, g_send, g_recv, h_send,
):
    n = Z * X
    dp = lax.axis_index("dp")
    ex = lax.axis_index("expert")
    z, x = dp // X, dp % X
    chunk = share // CHUNKS
    piece = share // SENDS

    def at_dp(zz, xx):
        return (zz * X + xx, ex)

    def lanes(base, size):
        return pl.ds(pl.multiple_of(base, 128), size)

    pair = z + 1 - 2 * (z % 2)
    edge = jnp.logical_or(z == 0, z == Z - 1)
    inside = jnp.logical_not(edge)

    def own_copy(zz):
        return pltpu.make_async_copy(
            grads.at[:, lanes((zz * X + x) * share, share)], own.at[zz], own_sem.at[zz]
        )

    def side_copy(k):
        start = (z * X + (x + k) % X) * share + HALF * chunk
        return pltpu.make_async_copy(
            grads.at[:, lanes(start, HALF * chunk)], side.at[k - 1], own_sem.at[Z + k - 1]
        )

    states = [
        pltpu.make_async_copy(a, b, state_sem.at[i])
        for i, (a, b) in enumerate(((master_in, master), (first_in, first), (second_in, second)))
    ]

    barrier = pltpu.get_barrier_semaphore()

    def greet(device):
        pl.semaphore_signal(barrier, inc=1, device_id=device, device_id_type=MESH)

    for k in range(1, X):
        greet(at_dp(z, (x + k) % X))
    for k in range(1, E):
        greet((dp, (ex + k) % E))

    @pl.when(z > 0)
    def _():
        greet(at_dp(z - 1, x))

    @pl.when(z < Z - 1)
    def _():
        greet(at_dp(z + 1, x))

    pl.semaphore_wait(barrier, X + E - jnp.where(edge, 1, 0))

    def x_copy(zz, k, c):
        to = (x + k) % X
        return pltpu.make_async_remote_copy(
            src_ref=grads.at[:, lanes((zz * X + to) * share + c * chunk, chunk)],
            dst_ref=xr.at[zz, k - 1, :, lanes(c * chunk, chunk)],
            send_sem=x_send.at[zz, k - 1, c],
            recv_sem=x_recv.at[zz, k - 1, c],
            device_id=at_dp(z, to),
            device_id_type=MESH,
        )

    def p_copy(k, c):
        return pltpu.make_async_remote_copy(
            src_ref=grads.at[:, lanes((pair * X + (x + k) % X) * share + c * chunk, chunk)],
            dst_ref=pr.at[k - 1, :, lanes((c - HALF) * chunk, chunk)],
            send_sem=p_send.at[k - 1, c - HALF],
            recv_sem=p_recv.at[k - 1, c - HALF],
            device_id=at_dp(pair, x),
            device_id_type=MESH,
        )

    def q_copy(k, c):
        return pltpu.make_async_remote_copy(
            src_ref=xcode.at[k - 1, c - HALF],
            dst_ref=xc.at[k - 1, c - HALF],
            send_sem=q_send.at[k - 1, c - HALF],
            recv_sem=q_recv.at[k - 1, c - HALF],
            device_id=at_dp(z, (x + k) % X),
            device_id_type=MESH,
        )

    def r_copy(c):
        return pltpu.make_async_remote_copy(
            src_ref=grads.at[:, lanes((pair * X + x) * share + c * chunk, chunk)],
            dst_ref=raw.at[:, lanes((c - HALF) * chunk, chunk)],
            send_sem=r_send.at[c - HALF],
            recv_sem=r_recv.at[c - HALF],
            device_id=at_dp(pair, x),
            device_id_type=MESH,
        )

    def z_copy(zz, c):
        up = jnp.where(zz > z, 1, 0)
        return pltpu.make_async_remote_copy(
            src_ref=code.at[zz, c],
            dst_ref=chain.at[up, zz, c],
            send_sem=z_send.at[zz, c],
            recv_sem=z_recv.at[up, zz, c],
            device_id=at_dp(z - 1 + 2 * up, x),
            device_id_type=MESH,
        )

    def from_chain(up, zz, c):
        return pltpu.make_async_remote_copy(
            src_ref=code.at[zz, c],
            dst_ref=chain.at[up, zz, c],
            send_sem=z_send.at[zz, c],
            recv_sem=z_recv.at[up, zz, c],
            device_id=at_dp(z, (x + 1) % X),
            device_id_type=MESH,
        )

    def for_dest(k, act):
        @pl.when(z + k < Z)
        def _():
            act(z + k)

        if k:
            @pl.when(z - k >= 0)
            def _():
                act(z - k)

    def start_first(zz):
        own_copy(zz).start()
        near = jnp.logical_or(zz == z, zz == pair)

        def body(c, carry):
            for k in range(1, X):
                x_copy(zz, k, c).start()
            return carry

        lax.fori_loop(0, jnp.where(near, HALF, CHUNKS), body, 0)

    def over_late(act):
        def body(c, carry):
            act(c)
            return carry

        lax.fori_loop(HALF, CHUNKS, body, 0)

    @over_late
    def _(c):
        for k in range(1, X):
            p_copy(k, c).start()

    for k in range(Z - 1, -1, -1):
        for_dest(k, start_first)
    for k in range(1, X):
        side_copy(k).start()
    for s in states:
        s.start()

    def part(ref, c, b):
        return ref[:, lanes(c * chunk + b * BLOCK, BLOCK)].astype(F32)

    def unpack(ref, b):
        return decode(ref[:, lanes(b * BLOCK, BLOCK)], ref[:, pl.ds(chunk, 128)])

    def pack(ref, block_sum):
        def add(b, peak):
            total = block_sum(b)
            exact[:, lanes(b * BLOCK, BLOCK)] = total
            return jnp.maximum(peak, lane_peak(total))

        peak = lax.fori_loop(0, chunk // BLOCK, add, jnp.zeros((own.shape[1], 128), F32))
        peak = (jnp.maximum(peak, TINY) * 1.01).astype(jnp.bfloat16)
        ref[:, pl.ds(chunk, 128)] = peak
        scale = spread_lanes(SPAN / peak.astype(F32))

        def write(b, carry):
            where = lanes(b * BLOCK, BLOCK)
            ref[:, where] = encode(exact[:, where], scale)
            return carry

        lax.fori_loop(0, chunk // BLOCK, write, 0)

    def gather_sum(zz, c, with_x, ups):
        def block_sum(b):
            total = part(own.at[zz], c, b)
            if with_x:
                for k in range(1, X):
                    total = total + part(xr.at[zz, k - 1], c, b)
            for up in ups:
                total = total + unpack(chain.at[up, zz, c], b)
            return total

        return block_sum

    def hop(zz, c):
        late = jnp.logical_and(zz == pair, c >= HALF)
        up = jnp.where(zz > z, 1, 0)
        first = z == (1 - up) * (Z - 1)
        later = jnp.logical_not(first)

        @pl.when(jnp.logical_not(late))
        def _():
            for k in range(1, X):
                x_copy(zz, k, c).wait_recv()

        @pl.when(later)
        def _():
            from_chain(up, zz, c).wait_recv()

        @pl.when(jnp.logical_and(first, jnp.logical_not(late)))
        def _():
            pack(code.at[zz, c], gather_sum(zz, c, True, ()))

        @pl.when(jnp.logical_and(later, jnp.logical_not(late)))
        def _():
            pack(code.at[zz, c], gather_sum(zz, c, True, (up,)))

        @pl.when(jnp.logical_and(later, late))
        def _():
            pack(code.at[zz, c], gather_sum(zz, c, False, (up,)))

        @pl.when(jnp.logical_not(jnp.logical_and(first, late)))
        def _():
            z_copy(zz, c).start()

    for k in range(Z - 1, 0, -1):
        for_dest(k, lambda zz: own_copy(zz).wait())
        lower, upper = z - k >= 0, z + k < Z
        count = jnp.where(lower, 1, 0) + jnp.where(upper, 1, 0)

        def body(i, carry, k=k, upper=upper, count=count):
            goes_up = jnp.logical_and(upper, i % count == 0)
            hop(jnp.where(goes_up, z + k, z - k), i // count)
            return carry

        @pl.when(count > 0)
        def _(body=body, count=count):
            lax.fori_loop(0, CHUNKS * count, body, 0)

        if k == Z - 1:
            @pl.when(edge)
            def _():
                over_late(lambda c: r_copy(c).start())

            for j in range(1, X):
                side_copy(j).wait()

            @over_late
            def _(c):
                for j in range(1, X):
                    p_copy(j, c).wait_recv()
                    pack(
                        xcode.at[j - 1, c - HALF],
                        lambda b: part(side.at[j - 1], c - HALF, b) + part(pr.at[j - 1], c - HALF, b),
                    )
                    q_copy(j, c).start()

    own_copy(z).wait()
    squares[...] = jnp.zeros_like(squares)

    def finish_chunk(c, block_sum):
        def body(b, carry):
            mean = block_sum(b) / n
            mean_grad[:, lanes(c * chunk + b * BLOCK, BLOCK)] = mean
            return carry + mean * mean

        squares[...] = lax.fori_loop(0, chunk // BLOCK, body, squares[...])

    def late_sum(c, ups, with_raw):
        chained = gather_sum(z, c, False, ups)

        def block_sum(b):
            total = chained(b)
            for k in range(1, X):
                total = total + unpack(xc.at[k - 1, c - HALF], b)
            if with_raw:
                total = total + part(raw, c - HALF, b)
            return total

        return block_sum

    far = jnp.where(pair < z, 0, 1)
    far = jnp.where(edge, jnp.where(z == 0, 0, 1), far)
    raw_pair = jnp.logical_and(inside, jnp.logical_or(pair == 0, pair == Z - 1))
    both_pair = jnp.logical_and(inside, jnp.logical_not(raw_pair))

    def early_finish(c):
        for k in range(1, X):
            x_copy(z, k, c).wait_recv()

        @pl.when(edge)
        def _():
            from_chain(far, z, c).wait_recv()
            finish_chunk(c, gather_sum(z, c, True, (far,)))

        @pl.when(inside)
        def _():
            for up in range(2):
                from_chain(up, z, c).wait_recv()
            finish_chunk(c, gather_sum(z, c, True, (0, 1)))

    def late_finish(c):
        for k in range(1, X):
            q_copy(k, c).wait_recv()

        @pl.when(edge)
        def _():
            from_chain(far, z, c).wait_recv()
            finish_chunk(c, late_sum(c, (far,), False))

        @pl.when(raw_pair)
        def _():
            from_chain(far, z, c).wait_recv()
            r_copy(c).wait_recv()
            finish_chunk(c, late_sum(c, (far,), True))

        if Z > 4:
            @pl.when(both_pair)
            def _():
                for up in range(2):
                    from_chain(up, z, c).wait_recv()
                finish_chunk(c, late_sum(c, (0, 1), False))

    def finish(c, carry):
        early_finish(c)
        late_finish(c + HALF)
        return carry

    lax.fori_loop(0, HALF, finish, 0)

    sums = squares[...]
    while sums.shape[1] > 128:
        half = sums.shape[1] // 2
        sums = sums[:, :half] + sums[:, half:]
    norms[0] = jnp.sum(sums, axis=0, keepdims=True)
    everyone = n * E

    def n_copy(k):
        to = (dp * E + ex + k) % everyone
        return pltpu.make_async_remote_copy(
            src_ref=norms.at[0], dst_ref=norms.at[k],
            send_sem=n_send.at[k], recv_sem=n_recv.at[k],
            device_id=(to // E, to % E), device_id_type=MESH,
        )

    def over_others(act):
        def body(k, carry):
            act(k)
            return carry

        lax.fori_loop(1, everyone, body, 0)

    over_others(lambda k: n_copy(k).start())
    for s in states:
        s.wait()
    over_others(lambda k: n_copy(k).wait_recv())
    total = jnp.full((8, 128), jnp.sum(norms[...]), F32)
    clip_all = jnp.minimum(1.0, clip_limit / (jnp.sqrt(total) + norm_eps))
    clip_factor = jnp.max(clip_all)

    def g_copy(zz, c, way):
        where = lanes((zz * X + x) * share + c * piece, piece)
        if way < 2:
            target = at_dp(z + 1 if way == 0 else z - 1, x)
        else:
            target = at_dp(z, (x + way - 1) % X)
        return pltpu.make_async_remote_copy(
            src_ref=gathered.at[:, where], dst_ref=gathered.at[:, where],
            send_sem=g_send.at[way, zz, c], recv_sem=g_recv.at[zz * X + x, c],
            device_id=target, device_id_type=MESH,
        )

    def arrived(zz, xx, c):
        where = lanes((zz * X + xx) * share + c * piece, piece)
        pltpu.make_async_remote_copy(
            src_ref=gathered.at[:, where], dst_ref=gathered.at[:, where],
            send_sem=g_send.at[0, 0, c], recv_sem=g_recv.at[zz * X + xx, c],
            device_id=(dp, (ex + 1) % E), device_id_type=MESH,
        ).wait_recv()

    def h_copy(k, c):
        where = lanes((z * X + (x + k) % X) * share + c * piece, piece)
        return pltpu.make_async_remote_copy(
            src_ref=gathered.at[:, where], dst_ref=gathered.at[:, where],
            send_sem=h_send.at[k - 1, c], recv_sem=g_recv.at[z * X + (x + k) % X, c],
            device_id=at_dp(pair, x), device_id_type=MESH,
        )

    def along_x(zz, c, act):
        @pl.when(jnp.logical_or(zz != pair, c < SEND_HALF))
        def _():
            for k in range(1, X):
                act(g_copy(zz, c, k + 1))

    def update(c, carry):
        def body(b, inner):
            where = lanes(c * piece + b * BLOCK, BLOCK)
            m, f, s = adam_update(
                mean_grad[:, where], master[:, where], first[:, where], second[:, where], clip_factor
            )
            master[:, where] = m
            first[:, where] = f
            second[:, where] = s
            gathered[:, lanes(dp * share + c * piece + b * BLOCK, BLOCK)] = m.astype(jnp.bfloat16)
            return inner

        lax.fori_loop(0, piece // BLOCK, body, 0)

        @pl.when(z < Z - 1)
        def _():
            g_copy(z, c, 0).start()

        @pl.when(z > 0)
        def _():
            g_copy(z, c, 1).start()

        for k in range(1, X):
            g_copy(z, c, k + 1).start()
        return carry

    lax.fori_loop(0, SENDS, update, 0)

    for s in range(1, Z):
        def relay(c, carry, s=s):
            @pl.when(z - s >= 0)
            def _():
                arrived(z - s, x, c)

                @pl.when(z < Z - 1)
                def _():
                    g_copy(z - s, c, 0).start()

                along_x(z - s, c, lambda copy: copy.start())

            @pl.when(z + s < Z)
            def _():
                arrived(z + s, x, c)

                @pl.when(z > 0)
                def _():
                    g_copy(z + s, c, 1).start()

                along_x(z + s, c, lambda copy: copy.start())

            return carry

        lax.fori_loop(0, SENDS, relay, 0)

        if s == max(Z - 2, 1):
            def across(c, carry):
                for k in range(1, X):
                    arrived(z, (x + k) % X, c)
                    h_copy(k, c).start()
                return carry

            lax.fori_loop(SEND_HALF, SENDS, across, 0)

    def drain(c, carry):
        for zz in range(Z):
            near = jnp.logical_or(zz == z, zz == pair)

            @pl.when(jnp.logical_not(jnp.logical_and(near, c >= HALF)))
            def _():
                for k in range(1, X):
                    x_copy(zz, k, c).wait_send()

            direct = jnp.logical_and(jnp.logical_and(edge, zz == pair), c >= HALF)

            @pl.when(jnp.logical_and(zz != z, jnp.logical_not(direct)))
            def _():
                z_copy(zz, c).wait_send()

        @pl.when(c >= HALF)
        def _():
            for k in range(1, X):
                p_copy(k, c).wait_send()
                q_copy(k, c).wait_send()

        @pl.when(jnp.logical_and(c >= HALF, edge))
        def _():
            r_copy(c).wait_send()

        return carry

    lax.fori_loop(0, CHUNKS, drain, 0)
    over_others(lambda k: n_copy(k).wait_send())

    for s in range(Z):
        def collect(zz, s=s):
            def body(c, carry):
                for k in range(1, X):
                    arrived(zz, (x + k) % X, c)
                return carry

            lax.fori_loop(0, SEND_HALF if s == 0 else SENDS, body, 0)

        for_dest(s, collect)

    def drain_sends(c, carry):
        for zz in range(Z):
            along_x(zz, c, lambda copy: copy.wait_send())

            @pl.when(jnp.logical_and(zz <= z, z < Z - 1))
            def _():
                g_copy(zz, c, 0).wait_send()

            @pl.when(jnp.logical_and(zz >= z, z > 0))
            def _():
                g_copy(zz, c, 1).wait_send()

        @pl.when(c >= SEND_HALF)
        def _():
            for k in range(1, X):
                h_copy(k, c).wait_send()

        return carry

    lax.fori_loop(0, SENDS, drain_sends, 0)


def write_out(count, *refs):
    sources, targets, sem = refs[:count], refs[count : 2 * count], refs[2 * count]

    def copies(i):
        size = sources[i].shape[1] // PIECES
        for p in range(PIECES):
            where = pl.ds(p * size, size)
            yield pltpu.make_async_copy(sources[i].at[:, where], targets[i].at[:, where], sem.at[i, p])

    for i in range(count):
        for copy in copies(i):
            copy.start()
    for i in range(count):
        for copy in copies(i):
            copy.wait()


def split(count):
    rows = 1
    while rows * rows < count:
        rows *= 2
    return rows, count // rows


def shards(Z, X, E, local_grads, master_weights, first_moment, second_moment):
    layers, flat = local_grads.shape[2:]
    n = Z * X
    share = flat // n
    whole = pl.BlockSpec(memory_space=pltpu.HBM)
    piece = jax.ShapeDtypeStruct((layers, share), F32)
    dma = pltpu.SemaphoreType.DMA
    local = pl.BlockSpec(memory_space=pltpu.VMEM)
    shapes = (jax.ShapeDtypeStruct((layers, flat), jnp.bfloat16), piece, piece, piece)
    arrays = (local_grads[0, 0], master_weights[0], first_moment[0], second_moment[0])
    out_bytes = layers * (2 * flat + 3 * 4 * share)
    coded = share // CHUNKS + 128
    used_bytes = layers * share * (Z * (2 * X + 3 * 2) + 4 * X + 5) + out_bytes
    results = pl.pallas_call(
        functools.partial(kernel, Z, X, E, share),
        out_shape=shapes,
        in_specs=[whole] * 4,
        out_specs=(local,) * 4,
        scratch_shapes=[
            pltpu.VMEM((Z, layers, share), jnp.bfloat16),
            pltpu.VMEM((X - 1, layers, share // 2), jnp.bfloat16),
            pltpu.VMEM((Z, X - 1, layers, share), jnp.bfloat16),
            pltpu.VMEM((X - 1, layers, share // 2), jnp.bfloat16),
            pltpu.VMEM((X - 1, HALF, layers, coded), jnp.bfloat16),
            pltpu.VMEM((layers, share // 2), jnp.bfloat16),
            pltpu.VMEM((2, Z, CHUNKS, layers, coded), jnp.bfloat16),
            pltpu.VMEM((Z, CHUNKS, layers, coded), jnp.bfloat16),
            pltpu.VMEM((X - 1, HALF, layers, coded), jnp.bfloat16),
            pltpu.VMEM((layers, share // CHUNKS), F32),
            pltpu.VMEM((layers, share), F32),
            pltpu.VMEM((layers, BLOCK), F32),
            pltpu.VMEM((n * E, 1, 128), F32),
            dma((Z + X - 1,)), dma((3,)),
            dma((Z, X - 1, CHUNKS)), dma((Z, X - 1, CHUNKS)),
            dma((Z, CHUNKS)), dma((2, Z, CHUNKS)),
            dma((X - 1, HALF)), dma((X - 1, HALF)), dma((X - 1, HALF)), dma((X - 1, HALF)),
            dma((HALF,)), dma((HALF,)),
            dma((n * E,)), dma((n * E,)),
            dma((X + 1, Z, SENDS)), dma((n, SENDS)), dma((X - 1, SENDS)),
        ],
        compiler_params=pltpu.CompilerParams(
            collective_id=0, has_side_effects=True, vmem_limit_bytes=used_bytes + SPARE_BYTES
        ),
    )(*(pltpu.with_memory_space_constraint(a, pltpu.HBM) for a in arrays))
    results = pl.pallas_call(
        functools.partial(write_out, len(shapes)),
        out_shape=shapes,
        in_specs=[local] * 4,
        out_specs=(whole,) * 4,
        scratch_shapes=[dma((len(shapes), PIECES))],
        compiler_params=pltpu.CompilerParams(vmem_limit_bytes=out_bytes + SPARE_BYTES),
    )(*results)
    return tuple(r[None] for r in results)


def solution(mesh):
    Z, X = split(mesh.shape["dp"])
    moments = P("expert", None, "dp")
    return jax.shard_map(
        functools.partial(shards, Z, X, mesh.shape["expert"]),
        mesh=mesh,
        in_specs=(P("dp", "expert", None, None), moments, moments, moments),
        out_specs=(P("expert", None, None), moments, moments, moments),
        check_vma=False,
    )
```

```python
import functools

import jax
import jax.numpy as jnp
from jax import lax
from jax.experimental import pallas as pl
from jax.experimental.pallas import tpu as pltpu
from jax.sharding import PartitionSpec as P

beta_first = 0.9
beta_second = 0.95
correct_first = 1.0 - 0.9**10
correct_second = 1.0 - 0.95**10
learn_rate = 0.05
decay_rate = 0.1
clip_limit = 1.0
tiny_eps = 1e-08
norm_eps = 1e-06

MESH = pl.DeviceIdType.MESH
F32 = jnp.float32
CHUNKS = 4
HALF = CHUNKS // 2
CROSS = CHUNKS // 4
PIECES = 8
SPARE_BYTES = 4 * 1024 * 1024
BLOCK = 2048
SPAN = 250.0
TINY = 1e-35


def adam_update(gradient, master, first, second, clip_factor):
    scaled = clip_factor * gradient
    new_first = beta_first * first + (1.0 - beta_first) * scaled
    new_second = beta_second * second + (1.0 - beta_second) * scaled * scaled
    direction = new_first * (1.0 / correct_first) / (jnp.sqrt(new_second * (1.0 / correct_second)) + tiny_eps)
    new_master = master - learn_rate * (decay_rate * master + direction)
    return (new_master, new_first, new_second)


def spread_lanes(tile):
    return jnp.concatenate([tile] * (BLOCK // 128), axis=1)


def lane_peak(values):
    peak = jnp.abs(values)
    while peak.shape[1] > 128:
        half = peak.shape[1] // 2
        peak = jnp.maximum(peak[:, :half], peak[:, half:])
    return peak


def encode(values, scale):
    size = jnp.exp2(jnp.abs(values) * scale - SPAN / 2)
    return jnp.where(values < 0, -size, size).astype(jnp.bfloat16)


def decode(codes, peak):
    codes = codes.astype(F32)
    size = (jnp.log2(jnp.abs(codes)) + SPAN / 2) * spread_lanes(peak.astype(F32) / SPAN)
    return jnp.where(codes < 0, -size, size)


def kernel(
    Z, X, E, share,
    grads, master_in, first_in, second_in,
    gathered, master, first, second,
    own, side, xr, pr, xc, raw, chain, code, xcode, exact, mean_grad, squares, norms, coded_state, coded_grad,
    own_sem, state_sem, x_send, x_recv, z_send, z_recv,
    p_send, p_recv, q_send, q_recv, r_send, r_recv,
    n_send, n_recv, s_send, s_recv, e_send, e_recv, g_send, g_recv, h_send,
):
    n = Z * X
    dp = lax.axis_index("dp")
    ex = lax.axis_index("expert")
    z, x = dp // X, dp % X
    chunk = share // CHUNKS

    def at_dp(zz, xx):
        return (zz * X + xx, ex)

    def lanes(base, size):
        return pl.ds(pl.multiple_of(base, 128), size)

    pair = z + 1 - 2 * (z % 2)
    edge = jnp.logical_or(z == 0, z == Z - 1)
    inside = jnp.logical_not(edge)
    raw_pair = jnp.logical_and(inside, jnp.logical_or(pair == 0, pair == Z - 1))
    both_pair = jnp.logical_and(inside, jnp.logical_not(raw_pair))

    def own_copy(zz):
        return pltpu.make_async_copy(
            grads.at[:, lanes((zz * X + x) * share, share)], own.at[zz], own_sem.at[zz]
        )

    def side_copy(k):
        start = (z * X + (x + k) % X) * share + HALF * chunk
        return pltpu.make_async_copy(
            grads.at[:, lanes(start, HALF * chunk)], side.at[k - 1], own_sem.at[Z + k - 1]
        )

    states = [
        pltpu.make_async_copy(a, b, state_sem.at[i])
        for i, (a, b) in enumerate(((master_in, master), (first_in, first), (second_in, second)))
    ]

    barrier = pltpu.get_barrier_semaphore()

    def greet(device):
        pl.semaphore_signal(barrier, inc=1, device_id=device, device_id_type=MESH)

    for k in range(1, X):
        greet(at_dp(z, (x + k) % X))
    for k in range(1, E):
        greet((dp, (ex + k) % E))

    @pl.when(z > 0)
    def _():
        greet(at_dp(z - 1, x))

    @pl.when(z < Z - 1)
    def _():
        greet(at_dp(z + 1, x))

    pl.semaphore_wait(barrier, X + E - jnp.where(edge, 1, 0))

    def x_copy(zz, k, c):
        to = (x + k) % X
        return pltpu.make_async_remote_copy(
            src_ref=grads.at[:, lanes((zz * X + to) * share + c * chunk, chunk)],
            dst_ref=xr.at[zz, k - 1, :, lanes(c * chunk, chunk)],
            send_sem=x_send.at[zz, k - 1, c],
            recv_sem=x_recv.at[zz, k - 1, c],
            device_id=at_dp(z, to),
            device_id_type=MESH,
        )

    def p_copy(k, c):
        return pltpu.make_async_remote_copy(
            src_ref=grads.at[:, lanes((pair * X + (x + k) % X) * share + c * chunk, chunk)],
            dst_ref=pr.at[k - 1, :, lanes((c - HALF) * chunk, chunk)],
            send_sem=p_send.at[k - 1, c - HALF],
            recv_sem=p_recv.at[k - 1, c - HALF],
            device_id=at_dp(pair, x),
            device_id_type=MESH,
        )

    def q_copy(k, c):
        return pltpu.make_async_remote_copy(
            src_ref=xcode.at[k - 1, c - HALF],
            dst_ref=xc.at[k - 1, c - HALF],
            send_sem=q_send.at[k - 1, c - HALF],
            recv_sem=q_recv.at[k - 1, c - HALF],
            device_id=at_dp(z, (x + k) % X),
            device_id_type=MESH,
        )

    def r_copy(c):
        return pltpu.make_async_remote_copy(
            src_ref=grads.at[:, lanes((pair * X + x) * share + c * chunk, chunk)],
            dst_ref=raw.at[:, lanes((c - HALF) * chunk, chunk)],
            send_sem=r_send.at[c - HALF],
            recv_sem=r_recv.at[c - HALF],
            device_id=at_dp(pair, x),
            device_id_type=MESH,
        )

    def z_copy(zz, c):
        up = jnp.where(zz > z, 1, 0)
        return pltpu.make_async_remote_copy(
            src_ref=code.at[zz, c],
            dst_ref=chain.at[up, zz, c],
            send_sem=z_send.at[zz, c],
            recv_sem=z_recv.at[up, zz, c],
            device_id=at_dp(z - 1 + 2 * up, x),
            device_id_type=MESH,
        )

    def from_chain(up, zz, c):
        return pltpu.make_async_remote_copy(
            src_ref=code.at[zz, c],
            dst_ref=chain.at[up, zz, c],
            send_sem=z_send.at[zz, c],
            recv_sem=z_recv.at[up, zz, c],
            device_id=at_dp(z, (x + 1) % X),
            device_id_type=MESH,
        )

    def for_dest(k, act):
        @pl.when(z + k < Z)
        def _():
            act(z + k)

        if k:
            @pl.when(z - k >= 0)
            def _():
                act(z - k)

    def start_first(zz):
        own_copy(zz).start()
        near = jnp.logical_or(zz == z, zz == pair)

        def body(c, carry):
            for k in range(1, X):
                x_copy(zz, k, c).start()
            return carry

        lax.fori_loop(0, jnp.where(near, HALF, CHUNKS), body, 0)

    def over_late(act):
        def body(c, carry):
            act(c)
            return carry

        lax.fori_loop(HALF, CHUNKS, body, 0)

    @over_late
    def _(c):
        for k in range(1, X):
            p_copy(k, c).start()

    for k in range(Z - 1, -1, -1):
        for_dest(k, start_first)
    for k in range(1, X):
        side_copy(k).start()
    for s in states:
        s.start()

    def part(ref, c, b):
        return ref[:, lanes(c * chunk + b * BLOCK, BLOCK)].astype(F32)

    def unpack(ref, b):
        return decode(ref[:, lanes(b * BLOCK, BLOCK)], ref[:, pl.ds(chunk, 128)])

    def pack(ref, block_sum):
        def add(b, peak):
            total = block_sum(b)
            exact[:, lanes(b * BLOCK, BLOCK)] = total
            return jnp.maximum(peak, lane_peak(total))

        peak = lax.fori_loop(0, chunk // BLOCK, add, jnp.zeros((own.shape[1], 128), F32))
        peak = (jnp.maximum(peak, TINY) * 1.01).astype(jnp.bfloat16)
        ref[:, pl.ds(chunk, 128)] = peak
        scale = spread_lanes(SPAN / peak.astype(F32))

        def write(b, carry):
            where = lanes(b * BLOCK, BLOCK)
            ref[:, where] = encode(exact[:, where], scale)
            return carry

        lax.fori_loop(0, chunk // BLOCK, write, 0)

    def s_copy(j, i):
        return pltpu.make_async_remote_copy(
            src_ref=coded_state.at[j, i], dst_ref=coded_state.at[j, i],
            send_sem=s_send.at[j, i], recv_sem=s_recv.at[j, i],
            device_id=at_dp(pair, x), device_id_type=MESH,
        )

    def e_copy(i):
        return pltpu.make_async_remote_copy(
            src_ref=coded_grad.at[i], dst_ref=coded_grad.at[i],
            send_sem=e_send.at[i], recv_sem=e_recv.at[i],
            device_id=at_dp(pair, x), device_id_type=MESH,
        )

    for s in states:
        s.wait()

    @pl.when(raw_pair)
    def _():
        def send_state(i, carry):
            for j, ref in enumerate((master, first, second)):
                pack(coded_state.at[j, i], lambda b, ref=ref: part(ref, i * HALF, b))
                s_copy(j, i).start()
            return carry

        lax.fori_loop(0, 2, send_state, 0)

    def gather_sum(zz, c, with_x, ups):
        def block_sum(b):
            total = part(own.at[zz], c, b)
            if with_x:
                for k in range(1, X):
                    total = total + part(xr.at[zz, k - 1], c, b)
            for up in ups:
                total = total + unpack(chain.at[up, zz, c], b)
            return total

        return block_sum

    def hop(zz, c):
        late = jnp.logical_and(zz == pair, c >= HALF)
        up = jnp.where(zz > z, 1, 0)
        first = z == (1 - up) * (Z - 1)
        later = jnp.logical_not(first)

        @pl.when(jnp.logical_not(late))
        def _():
            for k in range(1, X):
                x_copy(zz, k, c).wait_recv()

        @pl.when(later)
        def _():
            from_chain(up, zz, c).wait_recv()

        @pl.when(jnp.logical_and(first, jnp.logical_not(late)))
        def _():
            pack(code.at[zz, c], gather_sum(zz, c, True, ()))

        @pl.when(jnp.logical_and(later, jnp.logical_not(late)))
        def _():
            pack(code.at[zz, c], gather_sum(zz, c, True, (up,)))

        @pl.when(jnp.logical_and(later, late))
        def _():
            pack(code.at[zz, c], gather_sum(zz, c, False, (up,)))

        @pl.when(jnp.logical_not(jnp.logical_and(first, late)))
        def _():
            z_copy(zz, c).start()

    for k in range(Z - 1, 0, -1):
        for_dest(k, lambda zz: own_copy(zz).wait())
        lower, upper = z - k >= 0, z + k < Z
        count = jnp.where(lower, 1, 0) + jnp.where(upper, 1, 0)

        def body(i, carry, k=k, upper=upper, count=count):
            goes_up = jnp.logical_and(upper, i % count == 0)
            hop(jnp.where(goes_up, z + k, z - k), i // count)
            return carry

        @pl.when(count > 0)
        def _(body=body, count=count):
            lax.fori_loop(0, CHUNKS * count, body, 0)

        if k == Z - 1:
            @pl.when(edge)
            def _():
                over_late(lambda c: r_copy(c).start())

            for j in range(1, X):
                side_copy(j).wait()

            @over_late
            def _(c):
                for j in range(1, X):
                    p_copy(j, c).wait_recv()
                    pack(
                        xcode.at[j - 1, c - HALF],
                        lambda b: part(side.at[j - 1], c - HALF, b) + part(pr.at[j - 1], c - HALF, b),
                    )
                    q_copy(j, c).start()

    own_copy(z).wait()
    squares[...] = jnp.zeros_like(squares)

    def finish_chunk(c, block_sum):
        def body(b, carry):
            mean = block_sum(b) * (1.0 / n)
            mean_grad[:, lanes(c * chunk + b * BLOCK, BLOCK)] = mean
            return carry + mean * mean

        squares[...] = lax.fori_loop(0, chunk // BLOCK, body, squares[...])

    def late_sum(c, ups, with_raw):
        chained = gather_sum(z, c, False, ups)

        def block_sum(b):
            total = chained(b)
            for k in range(1, X):
                total = total + unpack(xc.at[k - 1, c - HALF], b)
            if with_raw:
                total = total + part(raw, c - HALF, b)
            return total

        return block_sum

    far = jnp.where(pair < z, 0, 1)
    far = jnp.where(edge, jnp.where(z == 0, 0, 1), far)
    def early_finish(c):
        for k in range(1, X):
            x_copy(z, k, c).wait_recv()

        @pl.when(edge)
        def _():
            from_chain(far, z, c).wait_recv()
            finish_chunk(c, gather_sum(z, c, True, (far,)))

        @pl.when(inside)
        def _():
            for up in range(2):
                from_chain(up, z, c).wait_recv()
            finish_chunk(c, gather_sum(z, c, True, (0, 1)))

    def late_finish(c):
        for k in range(1, X):
            q_copy(k, c).wait_recv()

        @pl.when(edge)
        def _():
            from_chain(far, z, c).wait_recv()
            finish_chunk(c, late_sum(c, (far,), False))

        @pl.when(raw_pair)
        def _():
            from_chain(far, z, c).wait_recv()
            r_copy(c).wait_recv()
            finish_chunk(c, late_sum(c, (far,), True))

        if Z > 4:
            @pl.when(both_pair)
            def _():
                for up in range(2):
                    from_chain(up, z, c).wait_recv()
                finish_chunk(c, late_sum(c, (0, 1), False))

    def share_grad(i, now=True):
        @pl.when(jnp.logical_and(raw_pair, now))
        def _():
            pack(coded_grad.at[i], lambda b: part(mean_grad, i * HALF, b))
            e_copy(i).start()

    def finish(c, carry):
        early_finish(c)
        share_grad(0, c == 0)
        late_finish(c + HALF)
        return carry

    lax.fori_loop(0, HALF, finish, 0)

    sums = squares[...]
    while sums.shape[1] > 128:
        half = sums.shape[1] // 2
        sums = sums[:, :half] + sums[:, half:]
    norms[0] = jnp.sum(sums, axis=0, keepdims=True)
    dp_at = [(dp + i) % n for i in range(n)]
    ex_at = [(ex + j) % E for j in range(E)]
    others = sorted(
        [(i, j) for i in range(n) for j in range(E) if i + j], key=lambda o: min(o[0], n - o[0]), reverse=True
    )

    def n_copy(i, j):
        k = i * E + j
        return pltpu.make_async_remote_copy(
            src_ref=norms.at[0], dst_ref=norms.at[k],
            send_sem=n_send.at[k], recv_sem=n_recv.at[k],
            device_id=(dp_at[i], ex_at[j]), device_id_type=MESH,
        )

    def over_others(act):
        for i, j in others:
            act(n_copy(i, j))

    over_others(lambda copy: copy.start())
    share_grad(1)
    over_others(lambda copy: copy.wait_recv())
    total = jnp.full((8, 128), jnp.sum(norms[...]), F32)
    clip_all = jnp.minimum(1.0, clip_limit / (jnp.sqrt(total) + norm_eps))
    clip_factor = jnp.max(clip_all)

    def g_copy(zz, c, way):
        where = lanes((zz * X + x) * share + c * chunk, chunk)
        if way < 2:
            target = at_dp(z + 1 if way == 0 else z - 1, x)
        else:
            target = at_dp(z, (x + way - 1) % X)
        return pltpu.make_async_remote_copy(
            src_ref=gathered.at[:, where], dst_ref=gathered.at[:, where],
            send_sem=g_send.at[way, zz, c], recv_sem=g_recv.at[zz * X + x, c],
            device_id=target, device_id_type=MESH,
        )

    def arrived(zz, xx, c):
        where = lanes((zz * X + xx) * share + c * chunk, chunk)
        pltpu.make_async_remote_copy(
            src_ref=gathered.at[:, where], dst_ref=gathered.at[:, where],
            send_sem=g_send.at[0, 0, c], recv_sem=g_recv.at[zz * X + xx, c],
            device_id=(dp, (ex + 1) % E), device_id_type=MESH,
        ).wait_recv()

    def h_copy(k, c):
        where = lanes((z * X + (x + k) % X) * share + c * chunk, chunk)
        return pltpu.make_async_remote_copy(
            src_ref=gathered.at[:, where], dst_ref=gathered.at[:, where],
            send_sem=h_send.at[k - 1, c], recv_sem=g_recv.at[z * X + (x + k) % X, c],
            device_id=at_dp(pair, x), device_id_type=MESH,
        )

    def along_x(zz, c, act):
        @pl.when(jnp.logical_or(zz != pair, c < CROSS))
        def _():
            for k in range(1, X):
                act(g_copy(zz, c, k + 1))

    def doubled(zz, c):
        return jnp.logical_and(jnp.logical_and(edge, zz == pair), c % HALF == 0)

    maker = jnp.where(edge, pair, z)

    def make_params(i, carry):
        def body(b, inner):
            m, f, s = (unpack(coded_state.at[j, i], b) for j in range(3))
            m, f, s = adam_update(unpack(coded_grad.at[i], b), m, f, s, clip_factor)
            start = (maker * X + x) * share + i * HALF * chunk + b * BLOCK
            gathered[:, lanes(start, BLOCK)] = m.astype(jnp.bfloat16)
            return inner

        @pl.when(edge)
        def _():
            for j in range(3):
                s_copy(j, i).wait_recv()
            e_copy(i).wait_recv()

        lax.fori_loop(0, chunk // BLOCK, body, 0)
        return carry

    def update_chunk(c, with_params):
        def body(b, inner):
            where = lanes(c * chunk + b * BLOCK, BLOCK)
            m, f, s = adam_update(
                mean_grad[:, where], master[:, where], first[:, where], second[:, where], clip_factor
            )
            master[:, where] = m
            first[:, where] = f
            second[:, where] = s
            if with_params:
                gathered[:, lanes(dp * share + c * chunk + b * BLOCK, BLOCK)] = m.astype(jnp.bfloat16)
            return inner

        lax.fori_loop(0, chunk // BLOCK, body, 0)

    rest = CHUNKS - 2

    def in_turn(t):
        return jnp.where(t < rest, t + 1 + jnp.where(t + 1 >= HALF, 1, 0), (t - rest) * HALF)

    def update(t, carry):
        c = in_turn(t)
        made = jnp.logical_and(raw_pair, t >= rest)

        @pl.when(jnp.logical_and(jnp.logical_not(both_pair), t == rest))
        def _():
            lax.fori_loop(0, 2, make_params, 0)

        @pl.when(made)
        def _():
            update_chunk(c, False)

        @pl.when(jnp.logical_not(made))
        def _():
            update_chunk(c, True)

        @pl.when(jnp.logical_and(z < Z - 1, jnp.logical_not(jnp.logical_and(made, pair > z))))
        def _():
            g_copy(z, c, 0).start()

        @pl.when(jnp.logical_and(z > 0, jnp.logical_not(jnp.logical_and(made, pair < z))))
        def _():
            g_copy(z, c, 1).start()

        for k in range(1, X):
            g_copy(z, c, k + 1).start()
        return carry

    lax.fori_loop(0, CHUNKS, update, 0)

    for s in range(1, Z):
        def relay(t, carry, s=s):
            c = in_turn(t)

            @pl.when(z - s >= 0)
            def _():
                @pl.when(jnp.logical_not(doubled(z - s, c)))
                def _():
                    arrived(z - s, x, c)

                @pl.when(z < Z - 1)
                def _():
                    g_copy(z - s, c, 0).start()

                along_x(z - s, c, lambda copy: copy.start())

            @pl.when(z + s < Z)
            def _():
                @pl.when(jnp.logical_not(doubled(z + s, c)))
                def _():
                    arrived(z + s, x, c)

                @pl.when(z > 0)
                def _():
                    g_copy(z + s, c, 1).start()

                along_x(z + s, c, lambda copy: copy.start())

            return carry

        lax.fori_loop(0, CHUNKS, relay, 0)

        if s == max(Z - 2, 1):
            def across(c, carry):
                for k in range(1, X):
                    arrived(z, (x + k) % X, c)
                    h_copy(k, c).start()
                return carry

            lax.fori_loop(CROSS, CHUNKS, across, 0)

    def drain(c, carry):
        for zz in range(Z):
            near = jnp.logical_or(zz == z, zz == pair)

            @pl.when(jnp.logical_not(jnp.logical_and(near, c >= HALF)))
            def _():
                for k in range(1, X):
                    x_copy(zz, k, c).wait_send()

            direct = jnp.logical_and(jnp.logical_and(edge, zz == pair), c >= HALF)

            @pl.when(jnp.logical_and(zz != z, jnp.logical_not(direct)))
            def _():
                z_copy(zz, c).wait_send()

        @pl.when(c >= HALF)
        def _():
            for k in range(1, X):
                p_copy(k, c).wait_send()
                q_copy(k, c).wait_send()

        @pl.when(jnp.logical_and(c >= HALF, edge))
        def _():
            r_copy(c).wait_send()

        return carry

    lax.fori_loop(0, CHUNKS, drain, 0)

    @pl.when(raw_pair)
    def _():
        for i in range(2):
            for j in range(3):
                s_copy(j, i).wait_send()
            e_copy(i).wait_send()

    over_others(lambda copy: copy.wait_send())

    for s in range(Z):
        def collect(zz, s=s):
            def body(c, carry):
                for k in range(1, X):
                    arrived(zz, (x + k) % X, c)
                return carry

            lax.fori_loop(0, CROSS if s == 0 else CHUNKS, body, 0)

        for_dest(s, collect)

    def drain_sends(c, carry):
        for zz in range(Z):
            along_x(zz, c, lambda copy: copy.wait_send())

            made = jnp.logical_and(jnp.logical_and(raw_pair, zz == z), c % HALF == 0)
            no_up, no_down = jnp.logical_and(made, pair > z), jnp.logical_and(made, pair < z)

            @pl.when(jnp.logical_and(jnp.logical_and(zz <= z, z < Z - 1), jnp.logical_not(no_up)))
            def _():
                g_copy(zz, c, 0).wait_send()

            @pl.when(jnp.logical_and(jnp.logical_and(zz >= z, z > 0), jnp.logical_not(no_down)))
            def _():
                g_copy(zz, c, 1).wait_send()

        @pl.when(c >= CROSS)
        def _():
            for k in range(1, X):
                h_copy(k, c).wait_send()

        return carry

    lax.fori_loop(0, CHUNKS, drain_sends, 0)


def write_out(count, *refs):
    sources, targets, sem = refs[:count], refs[count : 2 * count], refs[2 * count]

    def copies(i):
        size = sources[i].shape[1] // PIECES
        for p in range(PIECES):
            where = pl.ds(p * size, size)
            yield pltpu.make_async_copy(sources[i].at[:, where], targets[i].at[:, where], sem.at[i, p])

    for i in range(count):
        for copy in copies(i):
            copy.start()
    for i in range(count):
        for copy in copies(i):
            copy.wait()


def split(count):
    rows = 1
    while rows * rows < count:
        rows *= 2
    return rows, count // rows


def shards(Z, X, E, local_grads, master_weights, first_moment, second_moment):
    layers, flat = local_grads.shape[2:]
    n = Z * X
    share = flat // n
    whole = pl.BlockSpec(memory_space=pltpu.HBM)
    piece = jax.ShapeDtypeStruct((layers, share), F32)
    dma = pltpu.SemaphoreType.DMA
    local = pl.BlockSpec(memory_space=pltpu.VMEM)
    shapes = (jax.ShapeDtypeStruct((layers, flat), jnp.bfloat16), piece, piece, piece)
    arrays = (local_grads[0, 0], master_weights[0], first_moment[0], second_moment[0])
    out_bytes = layers * (2 * flat + 3 * 4 * share)
    coded = share // CHUNKS + 128
    used_bytes = layers * share * (Z * (2 * X + 3 * 2) + 4 * X + 9) + out_bytes
    results = pl.pallas_call(
        functools.partial(kernel, Z, X, E, share),
        out_shape=shapes,
        in_specs=[whole] * 4,
        out_specs=(local,) * 4,
        scratch_shapes=[
            pltpu.VMEM((Z, layers, share), jnp.bfloat16),
            pltpu.VMEM((X - 1, layers, share // 2), jnp.bfloat16),
            pltpu.VMEM((Z, X - 1, layers, share), jnp.bfloat16),
            pltpu.VMEM((X - 1, layers, share // 2), jnp.bfloat16),
            pltpu.VMEM((X - 1, HALF, layers, coded), jnp.bfloat16),
            pltpu.VMEM((layers, share // 2), jnp.bfloat16),
            pltpu.VMEM((2, Z, CHUNKS, layers, coded), jnp.bfloat16),
            pltpu.VMEM((Z, CHUNKS, layers, coded), jnp.bfloat16),
            pltpu.VMEM((X - 1, HALF, layers, coded), jnp.bfloat16),
            pltpu.VMEM((layers, share // CHUNKS), F32),
            pltpu.VMEM((layers, share), F32),
            pltpu.VMEM((layers, BLOCK), F32),
            pltpu.VMEM((n * E, 1, 128), F32),
            pltpu.VMEM((3, 2, layers, coded), jnp.bfloat16),
            pltpu.VMEM((2, layers, coded), jnp.bfloat16),
            dma((Z + X - 1,)), dma((3,)),
            dma((Z, X - 1, CHUNKS)), dma((Z, X - 1, CHUNKS)),
            dma((Z, CHUNKS)), dma((2, Z, CHUNKS)),
            dma((X - 1, HALF)), dma((X - 1, HALF)), dma((X - 1, HALF)), dma((X - 1, HALF)),
            dma((HALF,)), dma((HALF,)),
            dma((n * E,)), dma((n * E,)),
            dma((3, 2)), dma((3, 2)), dma((2,)), dma((2,)),
            dma((X + 1, Z, CHUNKS)), dma((n, CHUNKS)), dma((X - 1, CHUNKS)),
        ],
        compiler_params=pltpu.CompilerParams(
            collective_id=0, has_side_effects=True, vmem_limit_bytes=used_bytes + SPARE_BYTES
        ),
    )(*(pltpu.with_memory_space_constraint(a, pltpu.HBM) for a in arrays))
    results = pl.pallas_call(
        functools.partial(write_out, len(shapes)),
        out_shape=shapes,
        in_specs=[local] * 4,
        out_specs=(whole,) * 4,
        scratch_shapes=[dma((len(shapes), PIECES))],
        compiler_params=pltpu.CompilerParams(vmem_limit_bytes=out_bytes + SPARE_BYTES),
    )(*results)
    return tuple(r[None] for r in results)


def solution(mesh):
    Z, X = split(mesh.shape["dp"])
    moments = P("expert", None, "dp")
    return jax.shard_map(
        functools.partial(shards, Z, X, mesh.shape["expert"]),
        mesh=mesh,
        in_specs=(P("dp", "expert", None, None), moments, moments, moments),
        out_specs=(P("expert", None, None), moments, moments, moments),
        check_vma=False,
    )
```

```python
import functools

import jax
import jax.numpy as jnp
from jax import lax
from jax.experimental import pallas as pl
from jax.experimental.pallas import tpu as pltpu
from jax.sharding import PartitionSpec as P

beta_first = 0.9
beta_second = 0.95
correct_first = 1.0 - 0.9**10
correct_second = 1.0 - 0.95**10
learn_rate = 0.05
decay_rate = 0.1
clip_limit = 1.0
tiny_eps = 1e-08
norm_eps = 1e-06

MESH = pl.DeviceIdType.MESH
F32 = jnp.float32
CHUNKS = 4
HALF = CHUNKS // 2
EARLY = CHUNKS // 4
LATE = CHUNKS - EARLY
AHEAD = 4
PIECES = 8
SPARE_BYTES = 4 * 1024 * 1024
BLOCK = 2048
SPAN = 250.0
TINY = 1e-35


def adam_update(gradient, master, first, second, clip_factor):
    scaled = clip_factor * gradient
    new_first = beta_first * first + (1.0 - beta_first) * scaled
    new_second = beta_second * second + (1.0 - beta_second) * scaled * scaled
    direction = new_first * (1.0 / correct_first) / (jnp.sqrt(new_second * (1.0 / correct_second)) + tiny_eps)
    new_master = master - learn_rate * (decay_rate * master + direction)
    return (new_master, new_first, new_second)


def spread_lanes(tile):
    return jnp.concatenate([tile] * (BLOCK // 128), axis=1)


def lane_peak(values):
    peak = jnp.abs(values)
    while peak.shape[1] > 128:
        half = peak.shape[1] // 2
        peak = jnp.maximum(peak[:, :half], peak[:, half:])
    return peak


def encode(values, scale):
    size = jnp.exp2(jnp.abs(values) * scale - SPAN / 2)
    return jnp.where(values < 0, -size, size).astype(jnp.bfloat16)


def decode(codes, peak):
    codes = codes.astype(F32)
    size = (jnp.log2(jnp.abs(codes)) + SPAN / 2) * spread_lanes(peak.astype(F32) / SPAN)
    return jnp.where(codes < 0, -size, size)


def kernel(
    Z, X, E, share,
    grads, master_in, first_in, second_in,
    gathered, master, first, second,
    own, side, xr, pr, xc, raw, chain, code, xcode, exact, mean_grad, squares, norms, coded_state, coded_grad, made_grad,
    own_sem, state_sem, x_send, x_recv, z_send, z_recv,
    p_send, p_recv, q_send, q_recv, r_send, r_recv,
    n_send, n_recv, s_send, s_recv, e_send, e_recv, g_send, g_recv, h_send,
):
    n = Z * X
    dp = lax.axis_index("dp")
    ex = lax.axis_index("expert")
    z, x = dp // X, dp % X
    chunk = share // CHUNKS

    def at_dp(zz, xx):
        return (zz * X + xx, ex)

    def lanes(base, size):
        return pl.ds(pl.multiple_of(base, 128), size)

    pair = z + 1 - 2 * (z % 2)
    edge = jnp.logical_or(z == 0, z == Z - 1)
    inside = jnp.logical_not(edge)
    raw_pair = jnp.logical_and(inside, jnp.logical_or(pair == 0, pair == Z - 1))
    both_pair = jnp.logical_and(inside, jnp.logical_not(raw_pair))

    far = jnp.where(edge, jnp.where(z == 0, 0, 1), jnp.where(pair < z, 0, 1))
    rest = CHUNKS - 2

    def in_turn(t):
        return jnp.where(t < rest, t + 1 + jnp.where(t + 1 >= HALF, 1, 0), (t - rest) * HALF)

    def late_turn(t):
        return jnp.where(t == 0, HALF, t + jnp.where(t >= HALF, 1, 0))

    def chunk_turn(t):
        return jnp.where(t == 0, 0, late_turn(t - 1))

    def loop(low, high, act):
        def body(t, carry):
            act(t)
            return carry

        lax.fori_loop(low, high, body, 0)

    def own_copy(zz):
        return pltpu.make_async_copy(
            grads.at[:, lanes((zz * X + x) * share, share)], own.at[zz], own_sem.at[zz]
        )

    def side_copy(k):
        start = (z * X + (x + k) % X) * share + EARLY * chunk
        return pltpu.make_async_copy(
            grads.at[:, lanes(start, LATE * chunk)], side.at[k - 1], own_sem.at[Z + k - 1]
        )

    states = [
        pltpu.make_async_copy(a, b, state_sem.at[i])
        for i, (a, b) in enumerate(((master_in, master), (first_in, first), (second_in, second)))
    ]

    barrier = pltpu.get_barrier_semaphore()

    def greet(device):
        pl.semaphore_signal(barrier, inc=1, device_id=device, device_id_type=MESH)

    for k in range(1, X):
        greet(at_dp(z, (x + k) % X))
    for k in range(1, E):
        greet((dp, (ex + k) % E))

    @pl.when(z > 0)
    def _():
        greet(at_dp(z - 1, x))

    @pl.when(z < Z - 1)
    def _():
        greet(at_dp(z + 1, x))

    pl.semaphore_wait(barrier, X + E - jnp.where(edge, 1, 0))

    def x_copy(zz, k, c):
        to = (x + k) % X
        return pltpu.make_async_remote_copy(
            src_ref=grads.at[:, lanes((zz * X + to) * share + c * chunk, chunk)],
            dst_ref=xr.at[zz, k - 1, :, lanes(c * chunk, chunk)],
            send_sem=x_send.at[zz, k - 1, c],
            recv_sem=x_recv.at[zz, k - 1, c],
            device_id=at_dp(z, to),
            device_id_type=MESH,
        )

    def p_copy(k, c):
        return pltpu.make_async_remote_copy(
            src_ref=grads.at[:, lanes((pair * X + (x + k) % X) * share + c * chunk, chunk)],
            dst_ref=pr.at[k - 1, :, lanes((c - EARLY) * chunk, chunk)],
            send_sem=p_send.at[k - 1, c - EARLY],
            recv_sem=p_recv.at[k - 1, c - EARLY],
            device_id=at_dp(pair, x),
            device_id_type=MESH,
        )

    def q_copy(k, c):
        return pltpu.make_async_remote_copy(
            src_ref=xcode.at[k - 1, c - EARLY],
            dst_ref=xc.at[k - 1, c - EARLY],
            send_sem=q_send.at[k - 1, c - EARLY],
            recv_sem=q_recv.at[k - 1, c - EARLY],
            device_id=at_dp(z, (x + k) % X),
            device_id_type=MESH,
        )

    def slot(c):
        return c - 1 - jnp.where(c > HALF, 1, 0)

    def r_copy(c):
        return pltpu.make_async_remote_copy(
            src_ref=grads.at[:, lanes((pair * X + x) * share + c * chunk, chunk)],
            dst_ref=raw.at[:, lanes(slot(c) * chunk, chunk)],
            send_sem=r_send.at[slot(c)],
            recv_sem=r_recv.at[slot(c)],
            device_id=at_dp(pair, x),
            device_id_type=MESH,
        )

    def l_copy(c):
        toward = jnp.where(pair > z, 1, 0)
        return pltpu.make_async_remote_copy(
            src_ref=code.at[z, c],
            dst_ref=chain.at[toward, z, c],
            send_sem=z_send.at[z, c],
            recv_sem=z_recv.at[toward, z, c],
            device_id=at_dp(pair, x),
            device_id_type=MESH,
        )

    def z_copy(zz, c):
        up = jnp.where(zz > z, 1, 0)
        return pltpu.make_async_remote_copy(
            src_ref=code.at[zz, c],
            dst_ref=chain.at[up, zz, c],
            send_sem=z_send.at[zz, c],
            recv_sem=z_recv.at[up, zz, c],
            device_id=at_dp(z - 1 + 2 * up, x),
            device_id_type=MESH,
        )

    def from_chain(up, zz, c):
        return pltpu.make_async_remote_copy(
            src_ref=code.at[zz, c],
            dst_ref=chain.at[up, zz, c],
            send_sem=z_send.at[zz, c],
            recv_sem=z_recv.at[up, zz, c],
            device_id=at_dp(z, (x + 1) % X),
            device_id_type=MESH,
        )

    def for_dest(k, act):
        @pl.when(z + k < Z)
        def _():
            act(z + k)

        if k:
            @pl.when(z - k >= 0)
            def _():
                act(z - k)

    def start_first(zz):
        own_copy(zz).start()
        near = jnp.logical_or(zz == z, zz == pair)

        def body(c, carry):
            for k in range(1, X):
                x_copy(zz, k, chunk_turn(c)).start()
            return carry

        lax.fori_loop(0, jnp.where(near, EARLY, CHUNKS), body, 0)

    def send_side(t):
        for k in range(1, X):
            p_copy(k, late_turn(t)).start()

    loop(0, jnp.where(edge, 2, LATE), send_side)
    for k in range(Z - 1, 1, -1):
        for_dest(k, start_first)
    start_first(pair)

    @pl.when(inside)
    def _():
        start_first(2 * z - pair)

    start_first(z)
    for k in range(1, X):
        side_copy(k).start()
    for s in states:
        s.start()

    def part(ref, c, b):
        return ref[:, lanes(c * chunk + b * BLOCK, BLOCK)].astype(F32)

    def unpack(ref, b):
        return decode(ref[:, lanes(b * BLOCK, BLOCK)], ref[:, pl.ds(chunk, 128)])

    def pack(ref, block_sum):
        def add(b, peak):
            total = block_sum(b)
            exact[:, lanes(b * BLOCK, BLOCK)] = total
            return jnp.maximum(peak, lane_peak(total))

        peak = lax.fori_loop(0, chunk // BLOCK, add, jnp.zeros((own.shape[1], 128), F32))
        peak = (jnp.maximum(peak, TINY) * 1.01).astype(jnp.bfloat16)
        ref[:, pl.ds(chunk, 128)] = peak
        scale = spread_lanes(SPAN / peak.astype(F32))

        def write(b, carry):
            where = lanes(b * BLOCK, BLOCK)
            ref[:, where] = encode(exact[:, where], scale)
            return carry

        lax.fori_loop(0, chunk // BLOCK, write, 0)

    def s_copy(j, i):
        return pltpu.make_async_remote_copy(
            src_ref=coded_state.at[j, i], dst_ref=coded_state.at[j, i],
            send_sem=s_send.at[j, i], recv_sem=s_recv.at[j, i],
            device_id=at_dp(pair, x), device_id_type=MESH,
        )

    def e_copy(i):
        return pltpu.make_async_remote_copy(
            src_ref=coded_grad.at[i], dst_ref=coded_grad.at[i],
            send_sem=e_send.at[i], recv_sem=e_recv.at[i],
            device_id=at_dp(pair, x), device_id_type=MESH,
        )

    for s in states:
        s.wait()

    @pl.when(raw_pair)
    def _():
        def send_state(i, carry):
            for j, ref in enumerate((master, first, second)):
                pack(coded_state.at[j, i], lambda b, ref=ref: part(ref, i * HALF, b))

                @pl.when(i * 3 + j < AHEAD)
                def _(j=j):
                    s_copy(j, i).start()
            return carry

        lax.fori_loop(0, 2, send_state, 0)

    def gather_sum(zz, c, with_x, ups):
        def block_sum(b):
            total = part(own.at[zz], c, b)
            if with_x:
                for k in range(1, X):
                    total = total + part(xr.at[zz, k - 1], c, b)
            for up in ups:
                total = total + unpack(chain.at[up, zz, c], b)
            return total

        return block_sum

    def hop(zz, c):
        late = jnp.logical_and(zz == pair, c >= EARLY)
        up = jnp.where(zz > z, 1, 0)
        first = z == (1 - up) * (Z - 1)
        later = jnp.logical_not(first)
        sent = jnp.logical_not(jnp.logical_and(first, zz == pair))

        @pl.when(jnp.logical_and(sent, jnp.logical_not(late)))
        def _():
            for k in range(1, X):
                x_copy(zz, k, c).wait_recv()

        @pl.when(later)
        def _():
            from_chain(up, zz, c).wait_recv()

        @pl.when(jnp.logical_and(first, sent))
        def _():
            pack(code.at[zz, c], gather_sum(zz, c, True, ()))

        @pl.when(jnp.logical_and(later, jnp.logical_not(late)))
        def _():
            pack(code.at[zz, c], gather_sum(zz, c, True, (up,)))

        @pl.when(jnp.logical_and(later, late))
        def _():
            pack(code.at[zz, c], gather_sum(zz, c, False, (up,)))

        @pl.when(sent)
        def _():
            z_copy(zz, c).start()

    def send_pairs(t):
        c = late_turn(t)
        for j in range(1, X):
            p_copy(j, c).wait_recv()
            pack(
                xcode.at[j - 1, c - EARLY],
                lambda b: part(side.at[j - 1], c - EARLY, b) + part(pr.at[j - 1], c - EARLY, b),
            )
            q_copy(j, c).start()

    for k in range(Z - 1, 0, -1):
        for_dest(k, lambda zz: own_copy(zz).wait())
        lower, upper = z - k >= 0, z + k < Z
        count = jnp.where(lower, 1, 0) + jnp.where(upper, 1, 0)

        def body(i, carry, k=k, upper=upper, count=count):
            goes_up = jnp.logical_and(upper, i % count == 0)
            zz = jnp.where(goes_up, z + k, z - k)
            if k == 1:
                zz = jnp.where(i % count == 0, pair, 2 * z - pair)
            hop(zz, chunk_turn(i // count))
            return carry

        @pl.when(count > 0)
        def _(body=body, count=count):
            lax.fori_loop(0, CHUNKS * count, body, 0)

        if k == Z - 1:
            for j in range(1, X):
                side_copy(j).wait()
            loop(0, 2, send_pairs)

        if k == 2:
            @pl.when(edge)
            def _():
                loop(2, LATE, send_side)
                loop(0, rest, lambda t: r_copy(in_turn(t)).start())

    own_copy(z).wait()
    squares[...] = jnp.zeros_like(squares)

    def finish_chunk(c, block_sum, target=mean_grad):
        def body(b, carry):
            mean = block_sum(b) * (1.0 / n)
            target[:, lanes(c * chunk + b * BLOCK, BLOCK)] = mean
            return carry + mean * mean

        squares[...] = lax.fori_loop(0, chunk // BLOCK, body, squares[...])

    def late_sum(c, ups, with_raw):
        chained = gather_sum(z, c, False, ups)

        def block_sum(b):
            total = chained(b)
            for k in range(1, X):
                total = total + unpack(xc.at[k - 1, c - EARLY], b)
            if with_raw:
                total = total + part(raw, slot(c), b)
            return total

        return block_sum

    def early_finish(c):
        for k in range(1, X):
            x_copy(z, k, c).wait_recv()

        @pl.when(edge)
        def _():
            from_chain(far, z, c).wait_recv()
            finish_chunk(c, gather_sum(z, c, True, (far,)))

        @pl.when(raw_pair)
        def _():
            from_chain(far, z, c).wait_recv()
            pack(code.at[z, c], gather_sum(z, c, True, (far,)))
            l_copy(c).start()

        if Z > 4:
            @pl.when(both_pair)
            def _():
                for up in range(2):
                    from_chain(up, z, c).wait_recv()
                finish_chunk(c, gather_sum(z, c, True, (0, 1)))

    def late_finish(c):
        for k in range(1, X):
            q_copy(k, c).wait_recv()

        @pl.when(edge)
        def _():
            from_chain(far, z, c).wait_recv()
            finish_chunk(c, late_sum(c, (far,), False))

        @pl.when(jnp.logical_and(raw_pair, c == HALF))
        def _():
            from_chain(far, z, c).wait_recv()
            pack(code.at[z, c], late_sum(c, (far,), False))
            l_copy(c).start()

        @pl.when(jnp.logical_and(raw_pair, c != HALF))
        def _():
            from_chain(far, z, c).wait_recv()
            r_copy(c).wait_recv()
            finish_chunk(c, late_sum(c, (far,), True))

        if Z > 4:
            @pl.when(both_pair)
            def _():
                for up in range(2):
                    from_chain(up, z, c).wait_recv()
                finish_chunk(c, late_sum(c, (0, 1), False))

    def finish_for_pair(i, with_x):
        if with_x:
            for k in range(1, X):
                x_copy(pair, k, i * HALF).wait_recv()
        from_chain(far, pair, i * HALF).wait_recv()
        finish_chunk(0, gather_sum(pair, i * HALF, with_x, (far,)), made_grad.at[i])

    early_finish(0)
    loop(2, LATE, send_pairs)

    def finish(t, carry):
        late_finish(late_turn(t))

        @pl.when(jnp.logical_and(edge, t == 0))
        def _():
            finish_for_pair(0, True)

        @pl.when(jnp.logical_and(edge, t == 1))
        def _():
            finish_for_pair(1, False)

        return carry

    lax.fori_loop(0, LATE, finish, 0)

    sums = squares[...]
    while sums.shape[1] > 128:
        half = sums.shape[1] // 2
        sums = sums[:, :half] + sums[:, half:]
    norms[0] = jnp.sum(sums, axis=0, keepdims=True)
    dp_at = [(dp + i) % n for i in range(n)]
    ex_at = [(ex + j) % E for j in range(E)]
    others = sorted(
        [(i, j) for i in range(n) for j in range(E) if i + j], key=lambda o: min(o[0], n - o[0]), reverse=True
    )

    def n_copy(i, j):
        k = i * E + j
        return pltpu.make_async_remote_copy(
            src_ref=norms.at[0], dst_ref=norms.at[k],
            send_sem=n_send.at[k], recv_sem=n_recv.at[k],
            device_id=(dp_at[i], ex_at[j]), device_id_type=MESH,
        )

    def over_others(act):
        for i, j in others:
            act(n_copy(i, j))

    over_others(lambda copy: copy.start())

    @pl.when(edge)
    def _():
        def send_grad(i, carry):
            pack(coded_grad.at[i], lambda b: part(made_grad.at[i], 0, b))
            e_copy(i).start()
            return carry

        lax.fori_loop(0, 2, send_grad, 0)

    @pl.when(raw_pair)
    def _():
        for j in range(AHEAD - 3, 3):
            s_copy(j, 1).start()

    over_others(lambda copy: copy.wait_recv())
    total = jnp.full((8, 128), jnp.sum(norms[...]), F32)
    clip_all = jnp.minimum(1.0, clip_limit / (jnp.sqrt(total) + norm_eps))
    clip_factor = jnp.max(clip_all)

    def g_copy(zz, c, way):
        where = lanes((zz * X + x) * share + c * chunk, chunk)
        if way < 2:
            target = at_dp(z + 1 if way == 0 else z - 1, x)
        else:
            target = at_dp(z, (x + way - 1) % X)
        return pltpu.make_async_remote_copy(
            src_ref=gathered.at[:, where], dst_ref=gathered.at[:, where],
            send_sem=g_send.at[way, zz, c], recv_sem=g_recv.at[zz * X + x, c],
            device_id=target, device_id_type=MESH,
        )

    def arrived(zz, xx, c):
        where = lanes((zz * X + xx) * share + c * chunk, chunk)
        pltpu.make_async_remote_copy(
            src_ref=gathered.at[:, where], dst_ref=gathered.at[:, where],
            send_sem=g_send.at[0, 0, c], recv_sem=g_recv.at[zz * X + xx, c],
            device_id=(dp, (ex + 1) % E), device_id_type=MESH,
        ).wait_recv()

    def h_copy(k, c):
        where = lanes((z * X + (x + k) % X) * share + c * chunk, chunk)
        return pltpu.make_async_remote_copy(
            src_ref=gathered.at[:, where], dst_ref=gathered.at[:, where],
            send_sem=h_send.at[k - 1, c], recv_sem=g_recv.at[z * X + (x + k) % X, c],
            device_id=at_dp(pair, x), device_id_type=MESH,
        )

    def along_x(zz, c, act):
        @pl.when(jnp.logical_or(zz != pair, c < EARLY))
        def _():
            for k in range(1, X):
                act(g_copy(zz, c, k + 1))

    def doubled(zz, c):
        return jnp.logical_and(jnp.logical_and(edge, zz == pair), c % HALF == 0)

    maker = jnp.where(edge, pair, z)

    def make_params(i, carry):
        def body(b, inner):
            m, f, s = (unpack(coded_state.at[j, i], b) for j in range(3))
            m, f, s = adam_update(unpack(coded_grad.at[i], b), m, f, s, clip_factor)
            start = (maker * X + x) * share + i * HALF * chunk + b * BLOCK
            gathered[:, lanes(start, BLOCK)] = m.astype(jnp.bfloat16)
            return inner

        @pl.when(edge)
        def _():
            for j in range(3):
                s_copy(j, i).wait_recv()

        @pl.when(raw_pair)
        def _():
            e_copy(i).wait_recv()

        lax.fori_loop(0, chunk // BLOCK, body, 0)
        return carry

    def update_chunk(c, with_params):
        def body(b, inner):
            where = lanes(c * chunk + b * BLOCK, BLOCK)
            gradient = mean_grad[:, where] if with_params else unpack(coded_grad.at[c // HALF], b)
            m, f, s = adam_update(gradient, master[:, where], first[:, where], second[:, where], clip_factor)
            master[:, where] = m
            first[:, where] = f
            second[:, where] = s
            if with_params:
                gathered[:, lanes(dp * share + c * chunk + b * BLOCK, BLOCK)] = m.astype(jnp.bfloat16)
            return inner

        lax.fori_loop(0, chunk // BLOCK, body, 0)

    def update(t, carry):
        c = in_turn(t)
        made = jnp.logical_and(raw_pair, t >= rest)

        @pl.when(jnp.logical_and(jnp.logical_not(both_pair), t == rest))
        def _():
            lax.fori_loop(0, 2, make_params, 0)

        @pl.when(made)
        def _():
            update_chunk(c, False)

        @pl.when(jnp.logical_not(made))
        def _():
            update_chunk(c, True)

        @pl.when(jnp.logical_and(z < Z - 1, jnp.logical_not(jnp.logical_and(made, pair > z))))
        def _():
            g_copy(z, c, 0).start()

        @pl.when(jnp.logical_and(z > 0, jnp.logical_not(jnp.logical_and(made, pair < z))))
        def _():
            g_copy(z, c, 1).start()

        for k in range(1, X):
            g_copy(z, c, k + 1).start()
        return carry

    lax.fori_loop(0, CHUNKS, update, 0)

    for s in range(1, Z):
        def relay(t, carry, s=s):
            c = in_turn(t)

            @pl.when(z - s >= 0)
            def _():
                @pl.when(jnp.logical_not(doubled(z - s, c)))
                def _():
                    arrived(z - s, x, c)

                @pl.when(z < Z - 1)
                def _():
                    g_copy(z - s, c, 0).start()

                along_x(z - s, c, lambda copy: copy.start())

            @pl.when(z + s < Z)
            def _():
                @pl.when(jnp.logical_not(doubled(z + s, c)))
                def _():
                    arrived(z + s, x, c)

                @pl.when(z > 0)
                def _():
                    g_copy(z + s, c, 1).start()

                along_x(z + s, c, lambda copy: copy.start())

            return carry

        lax.fori_loop(0, CHUNKS, relay, 0)

        if s == max(Z - 2, 1):
            def across(c, carry):
                for k in range(1, X):
                    arrived(z, (x + k) % X, c)
                    h_copy(k, c).start()
                return carry

            lax.fori_loop(EARLY, CHUNKS, across, 0)

    def drain(c, carry):
        for zz in range(Z):
            near = jnp.logical_or(zz == z, zz == pair)

            @pl.when(jnp.logical_not(jnp.logical_and(near, c >= EARLY)))
            def _():
                for k in range(1, X):
                    x_copy(zz, k, c).wait_send()

            direct = jnp.logical_and(edge, zz == pair)

            @pl.when(jnp.logical_and(zz != z, jnp.logical_not(direct)))
            def _():
                z_copy(zz, c).wait_send()

        @pl.when(c >= EARLY)
        def _():
            for k in range(1, X):
                p_copy(k, c).wait_send()
                q_copy(k, c).wait_send()

        @pl.when(jnp.logical_and(c % HALF != 0, edge))
        def _():
            r_copy(c).wait_send()

        @pl.when(jnp.logical_and(c % HALF == 0, raw_pair))
        def _():
            l_copy(c).wait_send()

        return carry

    lax.fori_loop(0, CHUNKS, drain, 0)

    @pl.when(raw_pair)
    def _():
        for i in range(2):
            for j in range(3):
                s_copy(j, i).wait_send()

    @pl.when(edge)
    def _():
        for i in range(2):
            e_copy(i).wait_send()

    over_others(lambda copy: copy.wait_send())

    for s in range(Z):
        def collect(zz, s=s):
            def body(c, carry):
                for k in range(1, X):
                    arrived(zz, (x + k) % X, c)
                return carry

            lax.fori_loop(0, EARLY if s == 0 else CHUNKS, body, 0)

        for_dest(s, collect)

    def drain_sends(c, carry):
        for zz in range(Z):
            along_x(zz, c, lambda copy: copy.wait_send())

            made = jnp.logical_and(jnp.logical_and(raw_pair, zz == z), c % HALF == 0)
            no_up, no_down = jnp.logical_and(made, pair > z), jnp.logical_and(made, pair < z)

            @pl.when(jnp.logical_and(jnp.logical_and(zz <= z, z < Z - 1), jnp.logical_not(no_up)))
            def _():
                g_copy(zz, c, 0).wait_send()

            @pl.when(jnp.logical_and(jnp.logical_and(zz >= z, z > 0), jnp.logical_not(no_down)))
            def _():
                g_copy(zz, c, 1).wait_send()

        @pl.when(c >= EARLY)
        def _():
            for k in range(1, X):
                h_copy(k, c).wait_send()

        return carry

    lax.fori_loop(0, CHUNKS, drain_sends, 0)


def write_out(count, *refs):
    sources, targets, sem = refs[:count], refs[count : 2 * count], refs[2 * count]

    def copies(i):
        size = sources[i].shape[1] // PIECES
        for p in range(PIECES):
            where = pl.ds(p * size, size)
            yield pltpu.make_async_copy(sources[i].at[:, where], targets[i].at[:, where], sem.at[i, p])

    for i in range(count):
        for copy in copies(i):
            copy.start()
    for i in range(count):
        for copy in copies(i):
            copy.wait()


def split(count):
    rows = 1
    while rows * rows < count:
        rows *= 2
    return rows, count // rows


def shards(Z, X, E, local_grads, master_weights, first_moment, second_moment):
    layers, flat = local_grads.shape[2:]
    n = Z * X
    share = flat // n
    whole = pl.BlockSpec(memory_space=pltpu.HBM)
    piece = jax.ShapeDtypeStruct((layers, share), F32)
    dma = pltpu.SemaphoreType.DMA
    local = pl.BlockSpec(memory_space=pltpu.VMEM)
    shapes = (jax.ShapeDtypeStruct((layers, flat), jnp.bfloat16), piece, piece, piece)
    arrays = (local_grads[0, 0], master_weights[0], first_moment[0], second_moment[0])
    out_bytes = layers * (2 * flat + 3 * 4 * share)
    coded = share // CHUNKS + 128
    used_bytes = layers * share * (Z * (2 * X + 3 * 2) + 6 * X + 11) + out_bytes
    results = pl.pallas_call(
        functools.partial(kernel, Z, X, E, share),
        out_shape=shapes,
        in_specs=[whole] * 4,
        out_specs=(local,) * 4,
        scratch_shapes=[
            pltpu.VMEM((Z, layers, share), jnp.bfloat16),
            pltpu.VMEM((X - 1, layers, LATE * (share // CHUNKS)), jnp.bfloat16),
            pltpu.VMEM((Z, X - 1, layers, share), jnp.bfloat16),
            pltpu.VMEM((X - 1, layers, LATE * (share // CHUNKS)), jnp.bfloat16),
            pltpu.VMEM((X - 1, LATE, layers, coded), jnp.bfloat16),
            pltpu.VMEM((layers, share // 2), jnp.bfloat16),
            pltpu.VMEM((2, Z, CHUNKS, layers, coded), jnp.bfloat16),
            pltpu.VMEM((Z, CHUNKS, layers, coded), jnp.bfloat16),
            pltpu.VMEM((X - 1, LATE, layers, coded), jnp.bfloat16),
            pltpu.VMEM((layers, share // CHUNKS), F32),
            pltpu.VMEM((layers, share), F32),
            pltpu.VMEM((layers, BLOCK), F32),
            pltpu.VMEM((n * E, 1, 128), F32),
            pltpu.VMEM((3, 2, layers, coded), jnp.bfloat16),
            pltpu.VMEM((2, layers, coded), jnp.bfloat16),
            pltpu.VMEM((2, layers, share // CHUNKS), F32),
            dma((Z + X - 1,)), dma((3,)),
            dma((Z, X - 1, CHUNKS)), dma((Z, X - 1, CHUNKS)),
            dma((Z, CHUNKS)), dma((2, Z, CHUNKS)),
            dma((X - 1, LATE)), dma((X - 1, LATE)), dma((X - 1, LATE)), dma((X - 1, LATE)),
            dma((HALF,)), dma((HALF,)),
            dma((n * E,)), dma((n * E,)),
            dma((3, 2)), dma((3, 2)), dma((2,)), dma((2,)),
            dma((X + 1, Z, CHUNKS)), dma((n, CHUNKS)), dma((X - 1, CHUNKS)),
        ],
        compiler_params=pltpu.CompilerParams(
            collective_id=0, has_side_effects=True, vmem_limit_bytes=used_bytes + SPARE_BYTES
        ),
    )(*(pltpu.with_memory_space_constraint(a, pltpu.HBM) for a in arrays))
    results = pl.pallas_call(
        functools.partial(write_out, len(shapes)),
        out_shape=shapes,
        in_specs=[local] * 4,
        out_specs=(whole,) * 4,
        scratch_shapes=[dma((len(shapes), PIECES))],
        compiler_params=pltpu.CompilerParams(vmem_limit_bytes=out_bytes + SPARE_BYTES),
    )(*results)
    return tuple(r[None] for r in results)


def solution(mesh):
    Z, X = split(mesh.shape["dp"])
    moments = P("expert", None, "dp")
    return jax.shard_map(
        functools.partial(shards, Z, X, mesh.shape["expert"]),
        mesh=mesh,
        in_specs=(P("dp", "expert", None, None), moments, moments, moments),
        out_specs=(P("expert", None, None), moments, moments, moments),
        check_vma=False,
    )
```

```python
import functools

import jax
import jax.numpy as jnp
from jax import lax
from jax.experimental import pallas as pl
from jax.experimental.pallas import tpu as pltpu
from jax.sharding import PartitionSpec as P

beta_first = 0.9
beta_second = 0.95
correct_first = 1.0 - 0.9**10
correct_second = 1.0 - 0.95**10
learn_rate = 0.05
decay_rate = 0.1
clip_limit = 1.0
tiny_eps = 1e-08
norm_eps = 1e-06

MESH = pl.DeviceIdType.MESH
F32 = jnp.float32
CHUNKS = 4
HALF = CHUNKS // 2
EARLY = CHUNKS // 4
LATE = CHUNKS - EARLY
AHEAD = 4
PIECES = 8
SPARE_BYTES = 4 * 1024 * 1024
BLOCK = 4096
SPAN = 250.0
TINY = 1e-35


def adam_update(gradient, master, first, second, clip_factor):
    scaled = clip_factor * gradient
    new_first = beta_first * first + (1.0 - beta_first) * scaled
    new_second = beta_second * second + (1.0 - beta_second) * scaled * scaled
    direction = new_first * (1.0 / correct_first) / (jnp.sqrt(new_second * (1.0 / correct_second)) + tiny_eps)
    new_master = master - learn_rate * (decay_rate * master + direction)
    return (new_master, new_first, new_second)


def spread_lanes(tile):
    return jnp.concatenate([tile] * (BLOCK // 128), axis=1)


def lane_peak(values):
    peak = jnp.abs(values)
    while peak.shape[1] > 128:
        half = peak.shape[1] // 2
        peak = jnp.maximum(peak[:, :half], peak[:, half:])
    return peak


def encode(values, scale):
    size = jnp.exp2(jnp.abs(values) * scale - SPAN / 2)
    return jnp.where(values < 0, -size, size).astype(jnp.bfloat16)


def decode(codes, peak):
    codes = codes.astype(F32)
    size = (jnp.log2(jnp.abs(codes)) + SPAN / 2) * spread_lanes(peak.astype(F32) / SPAN)
    return jnp.where(codes < 0, -size, size)


def kernel(
    Z, X, E, share,
    grads, master_in, first_in, second_in,
    gathered, master, first, second,
    own, side, xr, pr, xc, raw, chain, code, xcode, exact, mean_grad, squares, norms, coded_state, coded_grad, made_grad,
    own_sem, state_sem, x_send, x_recv, z_send, z_recv,
    p_send, p_recv, q_send, q_recv, r_send, r_recv,
    n_send, n_recv, s_send, s_recv, e_send, e_recv, g_send, g_recv, h_send,
):
    n = Z * X
    dp = lax.axis_index("dp")
    ex = lax.axis_index("expert")
    z, x = dp // X, dp % X
    chunk = share // CHUNKS

    def at_dp(zz, xx):
        return (zz * X + xx, ex)

    def lanes(base, size):
        return pl.ds(pl.multiple_of(base, 128), size)

    pair = z + 1 - 2 * (z % 2)
    edge = jnp.logical_or(z == 0, z == Z - 1)
    inside = jnp.logical_not(edge)
    raw_pair = jnp.logical_and(inside, jnp.logical_or(pair == 0, pair == Z - 1))
    both_pair = jnp.logical_and(inside, jnp.logical_not(raw_pair))

    far = jnp.where(edge, jnp.where(z == 0, 0, 1), jnp.where(pair < z, 0, 1))
    rest = CHUNKS - 2

    def in_turn(t):
        return jnp.where(t < rest, t + 1 + jnp.where(t + 1 >= HALF, 1, 0), (t - rest) * HALF)

    def late_turn(t):
        return jnp.where(t == 0, HALF, t + jnp.where(t >= HALF, 1, 0))

    def chunk_turn(t):
        return jnp.where(t == 0, 0, late_turn(t - 1))

    def loop(low, high, act):
        def body(t, carry):
            act(t)
            return carry

        lax.fori_loop(low, high, body, 0)

    def own_copy(zz):
        return pltpu.make_async_copy(
            grads.at[:, lanes((zz * X + x) * share, share)], own.at[zz], own_sem.at[zz]
        )

    def side_copy(k):
        start = (z * X + (x + k) % X) * share + EARLY * chunk
        return pltpu.make_async_copy(
            grads.at[:, lanes(start, LATE * chunk)], side.at[k - 1], own_sem.at[Z + k - 1]
        )

    states = [
        pltpu.make_async_copy(a, b, state_sem.at[i])
        for i, (a, b) in enumerate(((master_in, master), (first_in, first), (second_in, second)))
    ]

    barrier = pltpu.get_barrier_semaphore()

    def greet(device):
        pl.semaphore_signal(barrier, inc=1, device_id=device, device_id_type=MESH)

    for k in range(1, X):
        greet(at_dp(z, (x + k) % X))
    for k in range(1, E):
        greet((dp, (ex + k) % E))

    @pl.when(z > 0)
    def _():
        greet(at_dp(z - 1, x))

    @pl.when(z < Z - 1)
    def _():
        greet(at_dp(z + 1, x))

    pl.semaphore_wait(barrier, X + E - jnp.where(edge, 1, 0))

    def x_copy(zz, k, c):
        to = (x + k) % X
        return pltpu.make_async_remote_copy(
            src_ref=grads.at[:, lanes((zz * X + to) * share + c * chunk, chunk)],
            dst_ref=xr.at[zz, k - 1, :, lanes(c * chunk, chunk)],
            send_sem=x_send.at[zz, k - 1, c],
            recv_sem=x_recv.at[zz, k - 1, c],
            device_id=at_dp(z, to),
            device_id_type=MESH,
        )

    def p_copy(k, c):
        return pltpu.make_async_remote_copy(
            src_ref=grads.at[:, lanes((pair * X + (x + k) % X) * share + c * chunk, chunk)],
            dst_ref=pr.at[k - 1, :, lanes((c - EARLY) * chunk, chunk)],
            send_sem=p_send.at[k - 1, c - EARLY],
            recv_sem=p_recv.at[k - 1, c - EARLY],
            device_id=at_dp(pair, x),
            device_id_type=MESH,
        )

    def q_copy(k, c):
        return pltpu.make_async_remote_copy(
            src_ref=xcode.at[k - 1, c - EARLY],
            dst_ref=xc.at[k - 1, c - EARLY],
            send_sem=q_send.at[k - 1, c - EARLY],
            recv_sem=q_recv.at[k - 1, c - EARLY],
            device_id=at_dp(z, (x + k) % X),
            device_id_type=MESH,
        )

    def slot(c):
        return c - 1 - jnp.where(c > HALF, 1, 0)

    def r_copy(c):
        return pltpu.make_async_remote_copy(
            src_ref=grads.at[:, lanes((pair * X + x) * share + c * chunk, chunk)],
            dst_ref=raw.at[:, lanes(slot(c) * chunk, chunk)],
            send_sem=r_send.at[slot(c)],
            recv_sem=r_recv.at[slot(c)],
            device_id=at_dp(pair, x),
            device_id_type=MESH,
        )

    def l_copy(c):
        toward = jnp.where(pair > z, 1, 0)
        return pltpu.make_async_remote_copy(
            src_ref=code.at[z, c],
            dst_ref=chain.at[toward, z, c],
            send_sem=z_send.at[z, c],
            recv_sem=z_recv.at[toward, z, c],
            device_id=at_dp(pair, x),
            device_id_type=MESH,
        )

    def z_copy(zz, c):
        up = jnp.where(zz > z, 1, 0)
        return pltpu.make_async_remote_copy(
            src_ref=code.at[zz, c],
            dst_ref=chain.at[up, zz, c],
            send_sem=z_send.at[zz, c],
            recv_sem=z_recv.at[up, zz, c],
            device_id=at_dp(z - 1 + 2 * up, x),
            device_id_type=MESH,
        )

    def from_chain(up, zz, c):
        return pltpu.make_async_remote_copy(
            src_ref=code.at[zz, c],
            dst_ref=chain.at[up, zz, c],
            send_sem=z_send.at[zz, c],
            recv_sem=z_recv.at[up, zz, c],
            device_id=at_dp(z, (x + 1) % X),
            device_id_type=MESH,
        )

    def for_dest(k, act):
        @pl.when(z + k < Z)
        def _():
            act(z + k)

        if k:
            @pl.when(z - k >= 0)
            def _():
                act(z - k)

    def start_first(zz):
        own_copy(zz).start()
        near = jnp.logical_or(zz == z, zz == pair)

        def body(c, carry):
            for k in range(1, X):
                x_copy(zz, k, chunk_turn(c)).start()
            return carry

        lax.fori_loop(0, jnp.where(near, EARLY, CHUNKS), body, 0)

    def send_side(t):
        for k in range(1, X):
            p_copy(k, late_turn(t)).start()

    loop(0, jnp.where(edge, 2, LATE), send_side)
    for k in range(Z - 1, 1, -1):
        for_dest(k, start_first)
    start_first(pair)

    @pl.when(inside)
    def _():
        start_first(2 * z - pair)

    start_first(z)
    for k in range(1, X):
        side_copy(k).start()
    for s in states:
        s.start()

    def part(ref, c, b):
        return ref[:, lanes(c * chunk + b * BLOCK, BLOCK)].astype(F32)

    def unpack(ref, b):
        return decode(ref[:, lanes(b * BLOCK, BLOCK)], ref[:, pl.ds(chunk, 128)])

    def pack(ref, block_sum):
        def add(b, peak):
            total = block_sum(b)
            exact[:, lanes(b * BLOCK, BLOCK)] = total
            return jnp.maximum(peak, lane_peak(total))

        peak = lax.fori_loop(0, chunk // BLOCK, add, jnp.zeros((own.shape[1], 128), F32))
        peak = (jnp.maximum(peak, TINY) * 1.01).astype(jnp.bfloat16)
        ref[:, pl.ds(chunk, 128)] = peak
        scale = spread_lanes(SPAN / peak.astype(F32))

        def write(b, carry):
            where = lanes(b * BLOCK, BLOCK)
            ref[:, where] = encode(exact[:, where], scale)
            return carry

        lax.fori_loop(0, chunk // BLOCK, write, 0)

    def s_copy(j, i):
        return pltpu.make_async_remote_copy(
            src_ref=coded_state.at[j, i], dst_ref=coded_state.at[j, i],
            send_sem=s_send.at[j, i], recv_sem=s_recv.at[j, i],
            device_id=at_dp(pair, x), device_id_type=MESH,
        )

    def e_copy(i):
        return pltpu.make_async_remote_copy(
            src_ref=coded_grad.at[i], dst_ref=coded_grad.at[i],
            send_sem=e_send.at[i], recv_sem=e_recv.at[i],
            device_id=at_dp(pair, x), device_id_type=MESH,
        )

    for s in states:
        s.wait()

    @pl.when(raw_pair)
    def _():
        def send_state(i, carry):
            for j, ref in enumerate((master, first, second)):
                pack(coded_state.at[j, i], lambda b, ref=ref: part(ref, i * HALF, b))

                @pl.when(i * 3 + j < AHEAD)
                def _(j=j):
                    s_copy(j, i).start()
            return carry

        lax.fori_loop(0, 2, send_state, 0)

    def gather_sum(zz, c, with_x, ups):
        def block_sum(b):
            total = part(own.at[zz], c, b)
            if with_x:
                for k in range(1, X):
                    total = total + part(xr.at[zz, k - 1], c, b)
            for up in ups:
                total = total + unpack(chain.at[up, zz, c], b)
            return total

        return block_sum

    def hop(zz, c):
        late = jnp.logical_and(zz == pair, c >= EARLY)
        up = jnp.where(zz > z, 1, 0)
        first = z == (1 - up) * (Z - 1)
        later = jnp.logical_not(first)
        sent = jnp.logical_not(jnp.logical_and(first, zz == pair))

        @pl.when(jnp.logical_and(sent, jnp.logical_not(late)))
        def _():
            for k in range(1, X):
                x_copy(zz, k, c).wait_recv()

        @pl.when(later)
        def _():
            from_chain(up, zz, c).wait_recv()

        @pl.when(jnp.logical_and(first, sent))
        def _():
            pack(code.at[zz, c], gather_sum(zz, c, True, ()))

        @pl.when(jnp.logical_and(later, jnp.logical_not(late)))
        def _():
            pack(code.at[zz, c], gather_sum(zz, c, True, (up,)))

        @pl.when(jnp.logical_and(later, late))
        def _():
            pack(code.at[zz, c], gather_sum(zz, c, False, (up,)))

        @pl.when(sent)
        def _():
            z_copy(zz, c).start()

    def send_pairs(t):
        c = late_turn(t)
        for j in range(1, X):
            p_copy(j, c).wait_recv()
            pack(
                xcode.at[j - 1, c - EARLY],
                lambda b: part(side.at[j - 1], c - EARLY, b) + part(pr.at[j - 1], c - EARLY, b),
            )
            q_copy(j, c).start()

    for k in range(Z - 1, 0, -1):
        for_dest(k, lambda zz: own_copy(zz).wait())
        lower, upper = z - k >= 0, z + k < Z
        count = jnp.where(lower, 1, 0) + jnp.where(upper, 1, 0)

        def body(i, carry, k=k, upper=upper, count=count):
            goes_up = jnp.logical_and(upper, i % count == 0)
            zz = jnp.where(goes_up, z + k, z - k)
            if k == 1:
                zz = jnp.where(i % count == 0, pair, 2 * z - pair)
            hop(zz, chunk_turn(i // count))
            return carry

        @pl.when(count > 0)
        def _(body=body, count=count):
            lax.fori_loop(0, CHUNKS * count, body, 0)

        if k == Z - 1:
            for j in range(1, X):
                side_copy(j).wait()
            loop(0, 2, send_pairs)

        if k == 2:
            @pl.when(edge)
            def _():
                loop(2, LATE, send_side)
                loop(0, rest, lambda t: r_copy(in_turn(t)).start())

    own_copy(z).wait()
    squares[...] = jnp.zeros_like(squares)

    def finish_chunk(c, block_sum, target=mean_grad):
        def body(b, carry):
            mean = block_sum(b) * (1.0 / n)
            target[:, lanes(c * chunk + b * BLOCK, BLOCK)] = mean
            return carry + mean * mean

        squares[...] = lax.fori_loop(0, chunk // BLOCK, body, squares[...])

    def late_sum(c, ups, with_raw):
        chained = gather_sum(z, c, False, ups)

        def block_sum(b):
            total = chained(b)
            for k in range(1, X):
                total = total + unpack(xc.at[k - 1, c - EARLY], b)
            if with_raw:
                total = total + part(raw, slot(c), b)
            return total

        return block_sum

    def early_finish(c):
        for k in range(1, X):
            x_copy(z, k, c).wait_recv()

        @pl.when(edge)
        def _():
            from_chain(far, z, c).wait_recv()
            finish_chunk(c, gather_sum(z, c, True, (far,)))

        @pl.when(raw_pair)
        def _():
            from_chain(far, z, c).wait_recv()
            pack(code.at[z, c], gather_sum(z, c, True, (far,)))
            l_copy(c).start()

        if Z > 4:
            @pl.when(both_pair)
            def _():
                for up in range(2):
                    from_chain(up, z, c).wait_recv()
                finish_chunk(c, gather_sum(z, c, True, (0, 1)))

    def late_finish(c):
        for k in range(1, X):
            q_copy(k, c).wait_recv()

        @pl.when(edge)
        def _():
            from_chain(far, z, c).wait_recv()
            finish_chunk(c, late_sum(c, (far,), False))

        @pl.when(jnp.logical_and(raw_pair, c == HALF))
        def _():
            from_chain(far, z, c).wait_recv()
            pack(code.at[z, c], late_sum(c, (far,), False))
            l_copy(c).start()

        @pl.when(jnp.logical_and(raw_pair, c != HALF))
        def _():
            from_chain(far, z, c).wait_recv()
            r_copy(c).wait_recv()
            finish_chunk(c, late_sum(c, (far,), True))

        if Z > 4:
            @pl.when(both_pair)
            def _():
                for up in range(2):
                    from_chain(up, z, c).wait_recv()
                finish_chunk(c, late_sum(c, (0, 1), False))

    def finish_for_pair(i, with_x):
        if with_x:
            for k in range(1, X):
                x_copy(pair, k, i * HALF).wait_recv()
        from_chain(far, pair, i * HALF).wait_recv()
        finish_chunk(0, gather_sum(pair, i * HALF, with_x, (far,)), made_grad.at[i])

    early_finish(0)
    loop(2, LATE, send_pairs)

    def finish(t, carry):
        late_finish(late_turn(t))

        @pl.when(jnp.logical_and(edge, t == 0))
        def _():
            finish_for_pair(0, True)

        @pl.when(jnp.logical_and(edge, t == 1))
        def _():
            finish_for_pair(1, False)

        return carry

    lax.fori_loop(0, LATE, finish, 0)

    sums = squares[...]
    while sums.shape[1] > 128:
        half = sums.shape[1] // 2
        sums = sums[:, :half] + sums[:, half:]
    norms[0] = jnp.sum(sums, axis=0, keepdims=True)
    dp_at = [(dp + i) % n for i in range(n)]
    ex_at = [(ex + j) % E for j in range(E)]
    others = sorted(
        [(i, j) for i in range(n) for j in range(E) if i + j], key=lambda o: min(o[0], n - o[0]), reverse=True
    )

    def n_copy(i, j):
        k = i * E + j
        return pltpu.make_async_remote_copy(
            src_ref=norms.at[0], dst_ref=norms.at[k],
            send_sem=n_send.at[k], recv_sem=n_recv.at[k],
            device_id=(dp_at[i], ex_at[j]), device_id_type=MESH,
        )

    def over_others(act):
        for i, j in others:
            act(n_copy(i, j))

    over_others(lambda copy: copy.start())

    @pl.when(edge)
    def _():
        def send_grad(i, carry):
            pack(coded_grad.at[i], lambda b: part(made_grad.at[i], 0, b))
            e_copy(i).start()
            return carry

        lax.fori_loop(0, 2, send_grad, 0)

    @pl.when(raw_pair)
    def _():
        for j in range(AHEAD - 3, 3):
            s_copy(j, 1).start()

    over_others(lambda copy: copy.wait_recv())
    total = jnp.full((8, 128), jnp.sum(norms[...]), F32)
    clip_all = jnp.minimum(1.0, clip_limit / (jnp.sqrt(total) + norm_eps))
    clip_factor = jnp.max(clip_all)

    def g_copy(zz, c, way):
        where = lanes((zz * X + x) * share + c * chunk, chunk)
        if way < 2:
            target = at_dp(z + 1 if way == 0 else z - 1, x)
        else:
            target = at_dp(z, (x + way - 1) % X)
        return pltpu.make_async_remote_copy(
            src_ref=gathered.at[:, where], dst_ref=gathered.at[:, where],
            send_sem=g_send.at[way, zz, c], recv_sem=g_recv.at[zz * X + x, c],
            device_id=target, device_id_type=MESH,
        )

    def arrived(zz, xx, c):
        where = lanes((zz * X + xx) * share + c * chunk, chunk)
        pltpu.make_async_remote_copy(
            src_ref=gathered.at[:, where], dst_ref=gathered.at[:, where],
            send_sem=g_send.at[0, 0, c], recv_sem=g_recv.at[zz * X + xx, c],
            device_id=(dp, (ex + 1) % E), device_id_type=MESH,
        ).wait_recv()

    def h_copy(k, c):
        where = lanes((z * X + (x + k) % X) * share + c * chunk, chunk)
        return pltpu.make_async_remote_copy(
            src_ref=gathered.at[:, where], dst_ref=gathered.at[:, where],
            send_sem=h_send.at[k - 1, c], recv_sem=g_recv.at[z * X + (x + k) % X, c],
            device_id=at_dp(pair, x), device_id_type=MESH,
        )

    def along_x(zz, c, act):
        @pl.when(jnp.logical_or(zz != pair, c < EARLY))
        def _():
            for k in range(1, X):
                act(g_copy(zz, c, k + 1))

    def doubled(zz, c):
        return jnp.logical_and(jnp.logical_and(edge, zz == pair), c % HALF == 0)

    maker = jnp.where(edge, pair, z)

    def make_params(i, carry):
        def body(b, inner):
            m, f, s = (unpack(coded_state.at[j, i], b) for j in range(3))
            m, f, s = adam_update(unpack(coded_grad.at[i], b), m, f, s, clip_factor)
            start = (maker * X + x) * share + i * HALF * chunk + b * BLOCK
            gathered[:, lanes(start, BLOCK)] = m.astype(jnp.bfloat16)
            return inner

        @pl.when(edge)
        def _():
            for j in range(3):
                s_copy(j, i).wait_recv()

        @pl.when(raw_pair)
        def _():
            e_copy(i).wait_recv()

        lax.fori_loop(0, chunk // BLOCK, body, 0)
        return carry

    def update_chunk(c, with_params):
        def body(b, inner):
            where = lanes(c * chunk + b * BLOCK, BLOCK)
            gradient = mean_grad[:, where] if with_params else unpack(coded_grad.at[c // HALF], b)
            m, f, s = adam_update(gradient, master[:, where], first[:, where], second[:, where], clip_factor)
            master[:, where] = m
            first[:, where] = f
            second[:, where] = s
            if with_params:
                gathered[:, lanes(dp * share + c * chunk + b * BLOCK, BLOCK)] = m.astype(jnp.bfloat16)
            return inner

        lax.fori_loop(0, chunk // BLOCK, body, 0)

    def update(t, carry):
        c = in_turn(t)
        made = jnp.logical_and(raw_pair, t >= rest)

        @pl.when(jnp.logical_and(jnp.logical_not(both_pair), t == rest))
        def _():
            lax.fori_loop(0, 2, make_params, 0)

        @pl.when(made)
        def _():
            update_chunk(c, False)

        @pl.when(jnp.logical_not(made))
        def _():
            update_chunk(c, True)

        @pl.when(jnp.logical_and(z < Z - 1, jnp.logical_not(jnp.logical_and(made, pair > z))))
        def _():
            g_copy(z, c, 0).start()

        @pl.when(jnp.logical_and(z > 0, jnp.logical_not(jnp.logical_and(made, pair < z))))
        def _():
            g_copy(z, c, 1).start()

        for k in range(1, X):
            g_copy(z, c, k + 1).start()
        return carry

    lax.fori_loop(0, CHUNKS, update, 0)

    for s in range(1, Z):
        def relay(t, carry, s=s):
            c = in_turn(t)

            @pl.when(z - s >= 0)
            def _():
                @pl.when(jnp.logical_not(doubled(z - s, c)))
                def _():
                    arrived(z - s, x, c)

                @pl.when(z < Z - 1)
                def _():
                    g_copy(z - s, c, 0).start()

                along_x(z - s, c, lambda copy: copy.start())

            @pl.when(z + s < Z)
            def _():
                @pl.when(jnp.logical_not(doubled(z + s, c)))
                def _():
                    arrived(z + s, x, c)

                @pl.when(z > 0)
                def _():
                    g_copy(z + s, c, 1).start()

                along_x(z + s, c, lambda copy: copy.start())

            return carry

        lax.fori_loop(0, CHUNKS, relay, 0)

        if s == max(Z - 2, 1):
            def across(c, carry):
                for k in range(1, X):
                    arrived(z, (x + k) % X, c)
                    h_copy(k, c).start()
                return carry

            lax.fori_loop(EARLY, CHUNKS, across, 0)

    def drain(c, carry):
        for zz in range(Z):
            near = jnp.logical_or(zz == z, zz == pair)

            @pl.when(jnp.logical_not(jnp.logical_and(near, c >= EARLY)))
            def _():
                for k in range(1, X):
                    x_copy(zz, k, c).wait_send()

            direct = jnp.logical_and(edge, zz == pair)

            @pl.when(jnp.logical_and(zz != z, jnp.logical_not(direct)))
            def _():
                z_copy(zz, c).wait_send()

        @pl.when(c >= EARLY)
        def _():
            for k in range(1, X):
                p_copy(k, c).wait_send()
                q_copy(k, c).wait_send()

        @pl.when(jnp.logical_and(c % HALF != 0, edge))
        def _():
            r_copy(c).wait_send()

        @pl.when(jnp.logical_and(c % HALF == 0, raw_pair))
        def _():
            l_copy(c).wait_send()

        return carry

    lax.fori_loop(0, CHUNKS, drain, 0)

    @pl.when(raw_pair)
    def _():
        for i in range(2):
            for j in range(3):
                s_copy(j, i).wait_send()

    @pl.when(edge)
    def _():
        for i in range(2):
            e_copy(i).wait_send()

    over_others(lambda copy: copy.wait_send())

    for s in range(Z):
        def collect(zz, s=s):
            def body(c, carry):
                for k in range(1, X):
                    arrived(zz, (x + k) % X, c)
                return carry

            lax.fori_loop(0, EARLY if s == 0 else CHUNKS, body, 0)

        for_dest(s, collect)

    def drain_sends(c, carry):
        for zz in range(Z):
            along_x(zz, c, lambda copy: copy.wait_send())

            made = jnp.logical_and(jnp.logical_and(raw_pair, zz == z), c % HALF == 0)
            no_up, no_down = jnp.logical_and(made, pair > z), jnp.logical_and(made, pair < z)

            @pl.when(jnp.logical_and(jnp.logical_and(zz <= z, z < Z - 1), jnp.logical_not(no_up)))
            def _():
                g_copy(zz, c, 0).wait_send()

            @pl.when(jnp.logical_and(jnp.logical_and(zz >= z, z > 0), jnp.logical_not(no_down)))
            def _():
                g_copy(zz, c, 1).wait_send()

        @pl.when(c >= EARLY)
        def _():
            for k in range(1, X):
                h_copy(k, c).wait_send()

        return carry

    lax.fori_loop(0, CHUNKS, drain_sends, 0)


def write_out(count, *refs):
    sources, targets, sem = refs[:count], refs[count : 2 * count], refs[2 * count]

    def copies(i):
        size = sources[i].shape[1] // PIECES
        for p in range(PIECES):
            where = pl.ds(p * size, size)
            yield pltpu.make_async_copy(sources[i].at[:, where], targets[i].at[:, where], sem.at[i, p])

    for i in range(count):
        for copy in copies(i):
            copy.start()
    for i in range(count):
        for copy in copies(i):
            copy.wait()


def split(count):
    rows = 1
    while rows * rows < count:
        rows *= 2
    return rows, count // rows


def shards(Z, X, E, local_grads, master_weights, first_moment, second_moment):
    layers, flat = local_grads.shape[2:]
    n = Z * X
    share = flat // n
    whole = pl.BlockSpec(memory_space=pltpu.HBM)
    piece = jax.ShapeDtypeStruct((layers, share), F32)
    dma = pltpu.SemaphoreType.DMA
    local = pl.BlockSpec(memory_space=pltpu.VMEM)
    shapes = (jax.ShapeDtypeStruct((layers, flat), jnp.bfloat16), piece, piece, piece)
    arrays = (local_grads[0, 0], master_weights[0], first_moment[0], second_moment[0])
    out_bytes = layers * (2 * flat + 3 * 4 * share)
    coded = share // CHUNKS + 128
    used_bytes = layers * share * (Z * (2 * X + 3 * 2) + 6 * X + 11) + out_bytes
    results = pl.pallas_call(
        functools.partial(kernel, Z, X, E, share),
        out_shape=shapes,
        in_specs=[whole] * 4,
        out_specs=(local,) * 4,
        scratch_shapes=[
            pltpu.VMEM((Z, layers, share), jnp.bfloat16),
            pltpu.VMEM((X - 1, layers, LATE * (share // CHUNKS)), jnp.bfloat16),
            pltpu.VMEM((Z, X - 1, layers, share), jnp.bfloat16),
            pltpu.VMEM((X - 1, layers, LATE * (share // CHUNKS)), jnp.bfloat16),
            pltpu.VMEM((X - 1, LATE, layers, coded), jnp.bfloat16),
            pltpu.VMEM((layers, share // 2), jnp.bfloat16),
            pltpu.VMEM((2, Z, CHUNKS, layers, coded), jnp.bfloat16),
            pltpu.VMEM((Z, CHUNKS, layers, coded), jnp.bfloat16),
            pltpu.VMEM((X - 1, LATE, layers, coded), jnp.bfloat16),
            pltpu.VMEM((layers, share // CHUNKS), F32),
            pltpu.VMEM((layers, share), F32),
            pltpu.VMEM((layers, BLOCK), F32),
            pltpu.VMEM((n * E, 1, 128), F32),
            pltpu.VMEM((3, 2, layers, coded), jnp.bfloat16),
            pltpu.VMEM((2, layers, coded), jnp.bfloat16),
            pltpu.VMEM((2, layers, share // CHUNKS), F32),
            dma((Z + X - 1,)), dma((3,)),
            dma((Z, X - 1, CHUNKS)), dma((Z, X - 1, CHUNKS)),
            dma((Z, CHUNKS)), dma((2, Z, CHUNKS)),
            dma((X - 1, LATE)), dma((X - 1, LATE)), dma((X - 1, LATE)), dma((X - 1, LATE)),
            dma((HALF,)), dma((HALF,)),
            dma((n * E,)), dma((n * E,)),
            dma((3, 2)), dma((3, 2)), dma((2,)), dma((2,)),
            dma((X + 1, Z, CHUNKS)), dma((n, CHUNKS)), dma((X - 1, CHUNKS)),
        ],
        compiler_params=pltpu.CompilerParams(
            collective_id=0, has_side_effects=True, vmem_limit_bytes=used_bytes + SPARE_BYTES
        ),
    )(*(pltpu.with_memory_space_constraint(a, pltpu.HBM) for a in arrays))
    results = pl.pallas_call(
        functools.partial(write_out, len(shapes)),
        out_shape=shapes,
        in_specs=[local] * 4,
        out_specs=(whole,) * 4,
        scratch_shapes=[dma((len(shapes), PIECES))],
        compiler_params=pltpu.CompilerParams(vmem_limit_bytes=out_bytes + SPARE_BYTES),
    )(*results)
    return tuple(r[None] for r in results)


def solution(mesh):
    Z, X = split(mesh.shape["dp"])
    moments = P("expert", None, "dp")
    return jax.shard_map(
        functools.partial(shards, Z, X, mesh.shape["expert"]),
        mesh=mesh,
        in_specs=(P("dp", "expert", None, None), moments, moments, moments),
        out_specs=(P("expert", None, None), moments, moments, moments),
        check_vma=False,
    )
```
